512 devices in a mesh: ens: 2 (over y), gx: 64 (over z, core), gy: 4 (over x).
Axes of the slice: x: 4, y: 2, z: 32, core: 2. Of those that a mesh axis runs over, the one named last changes fastest.
The devices are a block of a 4x16x32 slice.
Arguments:
- log_cond: float32 [1024, 512, 128], P(('ens', 'gx'), 'gy'), parts along dimension 0, may hold values from -1 to 1
- checkpoint: float32 [1024, 512, 128], P(('ens', 'gx'), 'gy'), parts along dimension 0, may hold values from 0 to 1
- survey: float32 [1024, 512, 128], P(('ens', 'gx'), 'gy'), parts along dimension 0, may hold values from 0 to 1
- survey_weight: float32 [1024, 512, 128], P(('ens', 'gx'), 'gy'), parts along dimension 0, may hold values from 0.5 to 5
- well_cells: int32 [512], P('ens'), parts along dimension 0, may hold values from 0 to 33554431
- well_data: float32 [512], P('ens'), parts along dimension 0, may hold values from 0 to 1
- well_weight: float32 [512], P('ens'), parts along dimension 0, may hold values from 1 to 10
- source_cells: int32 [128], P('ens'), parts along dimension 0, may hold values from 0 to 33554431
- source_rate: float32 [128], P('ens'), parts along dimension 0, may hold values from 5 to 20
- step_number: int32 [2], P('ens'), parts along dimension 0, may hold values from 0 to 1999
Outputs:
- log_cond_grad: float32 [1024, 512, 128], P(('ens', 'gx'), 'gy'), parts along dimension 0
- checkpoint_adjoint: float32 [1024, 512, 128], P(('ens', 'gx'), 'gy'), parts along dimension 0
- concentration: float32 [1024, 512, 128], P(('ens', 'gx'), 'gy'), parts along dimension 0
- misfit: float32 [2], P('ens'), parts along dimension 0
The draws below stay inside these ranges and needn't reach their ends.
There are 2 independent parts, one for each index of `ens`. The reference program is written for one: setup_inputs(seed, part) draws one part's arguments, and reference() takes and returns one part's arrays. A program takes and returns all parts, laid end to end along the dimension named above; each array names one. Nothing has to cross between parts.
Inputs may be any that keep to these rules, and one draw needn't show every extreme that they name: `well_cells`: flat cell index (x * 512 + y) * 128 + z. `source_cells`: flat cell index (x * 512 + y) * 128 + z.
All inputs are finite; a program needn't handle non-finite values.
Results may differ from the reference program's by a relative error of at most 0.00002.
Values sent between devices are 32-bit elements; how exact they have to be, the bound alone decides.
No kernel may reach another device: no remote copies, remote signals or barrier semaphores. Data moves between devices by JAX's collectives and lax.ppermute only.
A program may use at most 64 MiB of HBM per device.

```python
import math
import jax
import jax.numpy as jnp

NOBS = 256
NSRC = 64
NX = 512
NY = 512
NZ = 128


def place_ends(result, own_key, low, largest):
    longest = result.shape.index(max(result.shape))
    spots = []
    for shift in (0, 1):
        where = [jax.random.randint(jax.random.fold_in(own_key, axis), (), 0, length) for axis, length in enumerate(result.shape)]
        where[longest] = (where[longest] + shift) % result.shape[longest]
        spots.append(tuple(where))
    return result.at[spots[0]].set(low).at[spots[1]].set(largest)


def block_scale(key, extent, cuts, low, top_value):
    def one(position, parts):
        heights = jax.random.uniform(jax.random.fold_in(jax.random.fold_in(key, 6), position), (parts,), jnp.float32, low / len(cuts), top_value / len(cuts))
        return jnp.repeat(jnp.exp(heights), extent[position] // parts).reshape((-1,) + (1,) * (len(extent) - position - 1))

    level = one(*cuts[0])
    for cut in cuts[1:]:
        level = level * one(*cut)
    return level


def setup_inputs(seed: int = 0, part: int = 0) -> dict:
    seeds = jax.random.split(jax.random.key(seed), 11)
    own_keys = jax.random.split(jax.random.fold_in(seeds[10], part), 11)
    return {
        "log_cond": jnp.clip(jax.random.uniform(own_keys[0], (NX, NY, NZ), jnp.float32, -1.0, 1.0) * block_scale(own_keys[0], (NX, NY, NZ), ((0, 64), (1, 4)), -0.4, 0.0), -1.0, 1.0),
        "checkpoint": jnp.clip(1.0 * jax.random.uniform(own_keys[1], (NX, NY, NZ), jnp.float32) ** block_scale(own_keys[1], (NX, NY, NZ), ((0, 64), (1, 4)), -0.2, 0.2), 0.0, 1.0),
        "survey": jnp.clip(1.0 * jax.random.uniform(own_keys[2], (NX, NY, NZ), jnp.float32) ** block_scale(own_keys[2], (NX, NY, NZ), ((0, 64), (1, 4)), -0.2, 0.2), 0.0, 1.0),
        "survey_weight": jnp.clip(jnp.exp(math.log(5.0) - 2.3025851 * jax.random.uniform(own_keys[3], (NX, NY, NZ), jnp.float32) ** block_scale(own_keys[3], (NX, NY, NZ), ((0, 64), (1, 4)), -0.2, 0.2)), 0.5, 5.0),
        "well_cells": place_ends(jax.random.randint(own_keys[4], (NOBS,), 0, NX * NY * NZ), jax.random.fold_in(own_keys[4], 1), 0, (NX * NY * NZ) - 1).astype(jnp.int32),
        "well_data": jnp.clip(jax.random.uniform(own_keys[5], (NOBS,), jnp.float32, 0.0, 1.0), 0.0, 1.0),
        "well_weight": jnp.clip(jnp.exp(jax.random.uniform(own_keys[6], (NOBS,), jnp.float32, math.log(1.0), math.log(10.0))), 1.0, 10.0),
        "source_cells": place_ends(jax.random.randint(own_keys[7], (NSRC,), 0, NX * NY * NZ), jax.random.fold_in(own_keys[7], 1), 0, (NX * NY * NZ) - 1).astype(jnp.int32),
        "source_rate": jnp.clip(jax.random.uniform(own_keys[8], (NSRC,), jnp.float32, 5.0, 20.0), 5.0, 20.0),
        "step_number": jax.random.randint(own_keys[9], (1,), 0, 2000).astype(jnp.int32),
    }


time_step = 0.2
head_slope = 0.5
molecular = 0.05
dispersivity = 0.1

def step_forward(tracer, log_cond, source):
    cond_x = jnp.exp(0.5 * (log_cond[:-1] + log_cond[1:]))
    cond_y = jnp.exp(0.5 * (log_cond[:, :-1] + log_cond[:, 1:]))
    cond_z = jnp.exp(0.5 * (log_cond[:, :, :-1] + log_cond[:, :, 1:]))
    flux_x = head_slope * cond_x * tracer[:-1] - (molecular + dispersivity * cond_x) * (tracer[1:] - tracer[:-1])
    flux_y = -(molecular + dispersivity * cond_y) * (tracer[:, 1:] - tracer[:, :-1])
    flux_z = -(molecular + dispersivity * cond_z) * (tracer[:, :, 1:] - tracer[:, :, :-1])
    pad_x = jnp.pad(flux_x, ((1, 1), (0, 0), (0, 0)))
    pad_y = jnp.pad(flux_y, ((0, 0), (1, 1), (0, 0)))
    pad_z = jnp.pad(flux_z, ((0, 0), (0, 0), (1, 1)))
    spread = pad_x[1:] - pad_x[:-1] + (pad_y[:, 1:] - pad_y[:, :-1]) + (pad_z[:, :, 1:] - pad_z[:, :, :-1])
    return tracer - time_step * spread + time_step * source

def place(cells, values):
    blank = jnp.zeros((NX * NY * NZ,), jnp.float32)
    return blank.at[cells].add(values).reshape(NX, NY, NZ)

def reference(log_cond, checkpoint, survey, survey_weight, well_cells, well_data, well_weight, source_cells, source_rate, step_number):
    clock = step_number.astype(jnp.float32)[0]
    source_first = place(source_cells, source_rate * (1.0 + 0.5 * jnp.sin(0.05 * clock)))
    source_second = place(source_cells, source_rate * (1.0 + 0.5 * jnp.sin(0.05 * (clock + 1.0))))

    def objective(cond_field, start_field):
        middle = step_forward(start_field, cond_field, source_first)
        final = step_forward(middle, cond_field, source_second)
        missed = final - survey
        nearby = final.reshape(-1)[well_cells] - well_data
        value = 0.5 * jnp.sum(survey_weight * missed * missed) + 0.5 * jnp.sum(well_weight * nearby * nearby)
        return (value, final)
    value, pullback, final = jax.vjp(objective, log_cond, checkpoint, has_aux=True)
    grad_cond, grad_start = pullback(jnp.ones_like(value))
    misfit = (value / (NX * NY * NZ)).reshape(1)
    return (grad_cond, grad_start, final, misfit)
```

```python
import functools
import math
import operator

import jax
import jax.numpy as jnp
from jax import lax
from jax.experimental import pallas as pl
from jax.experimental.pallas import tpu as pltpu
from jax.sharding import Mesh
from jax.sharding import PartitionSpec as P

FAR = "gx_0"
GX = ("gx_0", "gx_1")
GY = "gy"
ENS_GX = ("ens", "gx_0", "gx_1")

time_step = 0.2
head_slope = 0.5
molecular = 0.05
dispersivity = 0.1

RIM = 3
ROW = 8

VMEM_WHOLE = pl.BlockSpec(memory_space=pltpu.VMEM)
SMEM_WHOLE = pl.BlockSpec(memory_space=pltpu.SMEM)


def split(value, size):
    if size & (size - 1) == 0:
        return value >> (size.bit_length() - 1), value & (size - 1)
    return lax.div(value, jnp.int32(size)), lax.rem(value, jnp.int32(size))


def place_in(axes):
    position = lax.axis_index(axes)
    return position, position % 2 == 0


def up(field, axis):
    return pltpu.roll(field, field.shape[axis] - 1, axis)


def down(field, axis):
    return pltpu.roll(field, 1, axis)


def lane_mask(shape):
    lane = lax.broadcasted_iota(jnp.int32, shape, 1)
    return jnp.where(lane < shape[1] - 1, jnp.float32(time_step), jnp.float32(0.0))


def row_mask(shape, first, total):
    position = lax.broadcasted_iota(jnp.int32, shape, 0) - ROW + first
    is_open = (position >= 0) & (position + 1 < total)
    return jnp.where(is_open, jnp.float32(time_step), jnp.float32(0.0))


def plane_mask(plane, first, total):
    position = first - RIM + plane
    is_open = (position >= 0) & (position + 1 < total)
    return jnp.where(is_open, jnp.float32(time_step), jnp.float32(0.0))


def visit(count, hit, act):
    group = math.gcd(count, 8)

    def one(base, inner):
        @pl.when(hit(base + inner))
        def _():
            act(base + inner)

    def step(index, carry):
        base = index * group
        anyone = functools.reduce(operator.or_, [hit(base + k) for k in range(group)])

        @pl.when(anyone)
        def _():
            lax.fori_loop(0, group, lambda k, c: (one(base, k), c)[1], 0)

        return carry

    lax.fori_loop(0, count // group, step, 0)


def pack_x_kernel(start_ref, cond_ref, one_ref, two_ref):
    size = start_ref.shape[0]
    _, even = place_in(GX)
    first = jnp.where(even, 0, size - RIM)
    second = size - RIM - first
    for k in range(RIM):
        one_ref[0, k] = start_ref[first + k]
        one_ref[1, k] = cond_ref[first + k]
        two_ref[0, k] = start_ref[second + k]
        two_ref[1, k] = cond_ref[second + k]


def pack_y_kernel(start_ref, cond_ref, x_one_ref, x_two_ref, one_ref, two_ref):
    size, rows = start_ref.shape[:2]
    _, even = place_in(GY)

    def fill(low_ref, high_ref):
        for out_ref, begin in ((low_ref, 0), (high_ref, rows - RIM)):
            span = slice(begin, begin + RIM)
            for which, own_ref in ((0, start_ref), (1, cond_ref)):
                out_ref[which, 0:RIM] = x_one_ref[which, :, span, :]
                out_ref[which, RIM : RIM + size] = own_ref[:, span, :]
                out_ref[which, RIM + size :] = x_two_ref[which, :, span, :]

    @pl.when(even)
    def _():
        fill(one_ref, two_ref)

    @pl.when(jnp.logical_not(even))
    def _():
        fill(two_ref, one_ref)


def pack_seed_kernel(seed_ref, x_one_ref, x_two_ref, one_ref, two_ref):
    size, rows = seed_ref.shape[:2]
    rim = RIM - 1
    _, even = place_in(GY)

    def fill(low_ref, high_ref):
        for out_ref, begin in ((low_ref, 0), (high_ref, rows - rim)):
            span = slice(begin, begin + rim)
            out_ref[0:rim] = x_one_ref[:, span, :]
            out_ref[rim : rim + size] = seed_ref[:, span, :]
            out_ref[rim + size :] = x_two_ref[:, span, :]

    @pl.when(even)
    def _():
        fill(one_ref, two_ref)

    @pl.when(jnp.logical_not(even))
    def _():
        fill(two_ref, one_ref)


def spread(wide_ref, rim, own, x_one, x_two, y_one, y_two):
    size, rows = own.shape
    shift = RIM - rim
    _, even_x = place_in(GX)
    _, even_y = place_in(GY)
    base_one = jnp.where(even_x, shift, RIM + size)
    base_two = shift + RIM + size - base_one

    def copy_own(k, carry):
        wide_ref[RIM + k, ROW : ROW + rows] = own(k)
        return carry

    lax.fori_loop(0, size, copy_own, 0)
    for k in range(rim):
        wide_ref[base_one + k, ROW : ROW + rows] = x_one(k)
        wide_ref[base_two + k, ROW : ROW + rows] = x_two(k)

    def edges(low, high):
        for k in range(size + 2 * rim):
            if k < rim:
                plane = base_one + k
            elif k < rim + size:
                plane = shift + k
            else:
                plane = base_two + k - rim - size
            wide_ref[plane, ROW - rim : ROW] = low(k)
            wide_ref[plane, ROW + rows : ROW + rows + rim] = high(k)

    @pl.when(even_y)
    def _():
        edges(y_one, y_two)

    @pl.when(jnp.logical_not(even_y))
    def _():
        edges(y_two, y_one)


class Own:
    def __init__(self, shape, read):
        self.shape = shape
        self.read = read

    def __call__(self, k):
        return self.read(k)


def forward_kernel(
    grid_x,
    grid_y,
    source_cells,
    first_rates,
    second_rates,
    well_cells,
    well_data,
    well_weight,
    start_ref,
    cond_ref,
    x_one_ref,
    x_two_ref,
    y_one_ref,
    y_two_ref,
    survey_ref,
    weight_ref,
    root_ref,
    state_ref,
    next_ref,
    final_ref,
    seed_ref,
    edge_one_ref,
    edge_two_ref,
    partial_ref,
    row_ref,
    flux_ref,
):
    size, rows, depth = start_ref.shape
    wide = (root_ref.shape[1], depth)
    place_x, even_x = place_in(GX)
    place_y, _ = place_in(GY)
    anchor_x = place_x * size
    anchor_y = place_y * rows

    spread(
        state_ref,
        RIM,
        Own((size, rows), lambda k: start_ref[k]),
        lambda k: x_one_ref[0, k],
        lambda k: x_two_ref[0, k],
        lambda k: y_one_ref[0, k],
        lambda k: y_two_ref[0, k],
    )
    spread(
        root_ref,
        RIM,
        Own((size, rows), lambda k: jnp.exp(0.5 * cond_ref[k])),
        lambda k: jnp.exp(0.5 * x_one_ref[1, k]),
        lambda k: jnp.exp(0.5 * x_two_ref[1, k]),
        lambda k: jnp.exp(0.5 * y_one_ref[1, k]),
        lambda k: jnp.exp(0.5 * y_two_ref[1, k]),
    )
    row_ref[...] = row_mask(wide, anchor_y, grid_y)
    open_z = lane_mask(wide)

    def along_x(ref, plane):
        here = ref[plane]
        ahead = ref[plane + 1]
        cond = root_ref[plane] * root_ref[plane + 1]
        flux = head_slope * cond * here - (molecular + dispersivity * cond) * (ahead - here)
        return flux * plane_mask(plane, anchor_x, grid_x)

    def advanced(ref, plane):
        here = ref[plane]
        root = root_ref[plane]
        flux_x = along_x(ref, plane)
        cond_y = root * up(root, 0)
        flux_y = (row_ref[...] * (molecular + dispersivity * cond_y)) * (here - up(here, 0))
        cond_z = root * up(root, 1)
        flux_z = (open_z * (molecular + dispersivity * cond_z)) * (here - up(here, 1))
        change = (flux_x - flux_ref[...]) + (flux_y - down(flux_y, 0)) + (flux_z - down(flux_z, 1))
        flux_ref[...] = flux_x
        return here - change

    def spot(cell):
        line, along_z = split(cell, depth)
        along_x_, along_y = split(line, grid_y)
        return along_x_ - anchor_x, along_y - anchor_y, along_z

    def within(cell, rim):
        at_x, at_y, _ = spot(cell)
        return (at_x >= -rim) & (at_x < size + rim) & (at_y >= -rim) & (at_y < rows + rim)

    lane = lax.broadcasted_iota(jnp.int32, (1, depth), 1)

    flux_ref[...] = along_x(state_ref, 0)

    def first_step(plane, carry):
        next_ref[plane] = advanced(state_ref, plane)
        return carry

    lax.fori_loop(1, size + 2 * RIM - 1, first_step, 0)

    def add_first(index):
        at_x, at_y, at_z = spot(source_cells[index])
        where = (at_x + RIM, pl.ds(at_y + ROW, 1), slice(None))
        amount = time_step * first_rates[index]
        next_ref[where] = next_ref[where] + jnp.where(lane == at_z, amount, 0.0)

    visit(source_cells.shape[0], lambda i: within(source_cells[i], RIM - 1), add_first)

    flux_ref[...] = along_x(next_ref, RIM - 1)

    def second_step(k, carry):
        final_ref[k] = advanced(next_ref, k + RIM)[ROW : ROW + rows]
        return carry

    lax.fori_loop(0, size, second_step, 0)

    def add_second(index):
        at_x, at_y, at_z = spot(source_cells[index])
        where = (at_x, pl.ds(at_y, 1), slice(None))
        amount = time_step * second_rates[index]
        final_ref[where] = final_ref[where] + jnp.where(lane == at_z, amount, 0.0)

    visit(source_cells.shape[0], lambda i: within(source_cells[i], 0), add_second)

    partial_ref[...] = jnp.zeros((1, depth), jnp.float32)

    def compare(k, total):
        missed = final_ref[k] - survey_ref[k]
        seed = weight_ref[k] * missed
        seed_ref[k] = seed
        return total + jnp.sum((seed * missed).reshape(rows // 8, 8, depth), axis=0)

    total = lax.fori_loop(0, size, compare, jnp.zeros((8, depth), jnp.float32))
    partial_ref[...] = jnp.sum(total, axis=0, keepdims=True)

    def observe(index):
        at_x, at_y, at_z = spot(well_cells[index])
        where = (at_x, pl.ds(at_y, 1), slice(None))
        nearby = final_ref[where] - well_data[index]
        pull = jnp.where(lane == at_z, well_weight[index] * nearby, 0.0)
        seed_ref[where] = seed_ref[where] + pull
        partial_ref[...] = partial_ref[...] + pull * nearby

    visit(well_cells.shape[0], lambda i: within(well_cells[i], 0), observe)

    rim = RIM - 1
    first = jnp.where(even_x, 0, size - rim)
    second = size - rim - first
    for k in range(rim):
        edge_one_ref[k] = seed_ref[first + k]
        edge_two_ref[k] = seed_ref[second + k]


def adjoint_kernel(
    grid_x,
    grid_y,
    root_ref,
    state_ref,
    next_ref,
    seed_ref,
    x_one_ref,
    x_two_ref,
    y_one_ref,
    y_two_ref,
    grad_ref,
    back_ref,
    last_ref,
    middle_ref,
    partial_ref,
    row_ref,
    pull_ref,
    sens_ref,
):
    size, rows, depth = seed_ref.shape
    wide = (root_ref.shape[1], depth)
    place_x, _ = place_in(GX)
    place_y, _ = place_in(GY)
    anchor_x = place_x * size
    anchor_y = place_y * rows
    spread(
        last_ref,
        RIM - 1,
        Own((size, rows), lambda k: seed_ref[k]),
        lambda k: x_one_ref[k],
        lambda k: x_two_ref[k],
        lambda k: y_one_ref[k],
        lambda k: y_two_ref[k],
    )
    row_ref[...] = row_mask(wide, anchor_y, grid_y)
    open_z = lane_mask(wide)

    def along_x(adjoint_ref, tracer_ref, plane):
        jump = plane_mask(plane, anchor_x, grid_x) * (adjoint_ref[plane + 1] - adjoint_ref[plane])
        cond = root_ref[plane] * root_ref[plane + 1]
        pull = jump * (molecular + dispersivity * cond)
        push = jump * (head_slope * cond) + pull
        here = tracer_ref[plane]
        rise = head_slope * here - dispersivity * (tracer_ref[plane + 1] - here)
        return push, pull, jump * rise * (0.5 * cond)

    def along(adjoint, tracer, root, is_open, axis):
        jump = is_open * (up(adjoint, axis) - adjoint)
        cond = root * up(root, axis)
        pull = jump * (molecular + dispersivity * cond)
        sens = (jump * (tracer - up(tracer, axis))) * ((0.5 * dispersivity) * cond)
        return pull - down(pull, axis), sens + down(sens, axis)

    def reversed_step(adjoint_ref, tracer_ref, plane):
        push, pull, sens = along_x(adjoint_ref, tracer_ref, plane)
        adjoint = adjoint_ref[plane]
        tracer = tracer_ref[plane]
        root = root_ref[plane]
        change_y, sens_y = along(adjoint, tracer, root, row_ref[...], 0)
        change_z, sens_z = along(adjoint, tracer, root, open_z, 1)
        updated = adjoint + (push - pull_ref[...]) + change_y + change_z
        gradient = (sens + sens_ref[...]) + sens_y + sens_z
        pull_ref[...] = pull
        sens_ref[...] = sens
        return updated, gradient

    def begin(adjoint_ref, tracer_ref, plane):
        _, pull, sens = along_x(adjoint_ref, tracer_ref, plane)
        pull_ref[...] = pull
        sens_ref[...] = sens

    begin(last_ref, next_ref, RIM - 2)

    def later(plane, carry):
        updated, gradient = reversed_step(last_ref, next_ref, plane)
        middle_ref[plane] = updated
        partial_ref[plane] = gradient
        return carry

    lax.fori_loop(RIM - 1, size + RIM + 1, later, 0)

    begin(middle_ref, state_ref, RIM - 1)

    def earlier(k, carry):
        updated, gradient = reversed_step(middle_ref, state_ref, k + RIM)
        back_ref[k] = updated[ROW : ROW + rows]
        grad_ref[k] = (gradient + partial_ref[k + RIM])[ROW : ROW + rows]
        return carry

    lax.fori_loop(0, size, earlier, 0)


def call(kernel, outs, operands, *, smem=0, scratch=(), flops=1_000_000, limit=2, name):
    shapes = tuple(
        pltpu.VMEM(shape, jnp.float32) if kept else jax.ShapeDtypeStruct(shape, jnp.float32)
        for shape, kept in outs
    )
    operands = operands[:smem] + tuple(
        pltpu.with_memory_space_constraint(operand, pltpu.VMEM) for operand in operands[smem:]
    )
    return pl.pallas_call(
        kernel,
        out_shape=shapes,
        in_specs=[SMEM_WHOLE] * smem + [VMEM_WHOLE] * (len(operands) - smem),
        out_specs=tuple(VMEM_WHOLE for _ in outs),
        scratch_shapes=[pltpu.VMEM(shape, jnp.float32) for shape in scratch],
        cost_estimate=pl.CostEstimate(flops=flops, transcendentals=0, bytes_accessed=1_000_000),
        compiler_params=pltpu.CompilerParams(vmem_limit_bytes=limit << 20),
        name=name,
    )(*operands)


def swapped(one, two, axes):
    count = lax.axis_size(axes)
    outer = [(i, i + 1) for i in range(1, count - 1, 2)]
    inner = [(i, i + 1) for i in range(0, count - 1, 2)]
    back = lambda pairs: pairs + [(b, a) for a, b in pairs]
    return lax.ppermute(one, axes, back(outer)), lax.ppermute(two, axes, back(inner))


def from_everyone(shard, axis):
    count = lax.axis_size(axis)
    return lax.all_to_all(
        jnp.broadcast_to(shard[None], (count, *shard.shape)), axis, 0, 0, tiled=True
    )


def on_device(
    log_cond,
    checkpoint,
    survey,
    survey_weight,
    well_cells,
    well_data,
    well_weight,
    source_cells,
    source_rate,
    step_number,
):
    size, rows, depth = checkpoint.shape
    grid_x = size * lax.axis_size(GX)
    grid_y = rows * lax.axis_size(GY)
    clock = step_number.astype(jnp.float32)[0]
    first_rates = source_rate * (1.0 + 0.5 * jnp.sin(0.05 * clock))
    second_rates = source_rate * (1.0 + 0.5 * jnp.sin(0.05 * (clock + 1.0)))

    planes = size + 2 * RIM
    wide = (planes, rows + 2 * ROW, depth)
    flat = wide[1:]
    block = (size, rows, depth)
    rim = RIM - 1

    x_edge = (2, RIM, rows, depth)
    x_one, x_two = call(pack_x_kernel, ((x_edge, True),) * 2, (checkpoint, log_cond), name="pack_x")
    x_one, x_two = swapped(x_one, x_two, GX)
    y_edge = (2, planes, RIM, depth)
    y_one, y_two = call(
        pack_y_kernel, ((y_edge, True),) * 2, (checkpoint, log_cond, x_one, x_two), name="pack_y"
    )
    y_one, y_two = swapped(y_one, y_two, GY)

    s_edge = (rim, rows, depth)
    root, state, later, final, seed, s_one, s_two, partial = call(
        functools.partial(forward_kernel, grid_x, grid_y),
        (
            (wide, True),
            (wide, True),
            (wide, True),
            (block, False),
            (block, True),
            (s_edge, True),
            (s_edge, True),
            ((1, depth), True),
        ),
        (
            source_cells,
            first_rates,
            second_rates,
            well_cells,
            well_data,
            well_weight,
            checkpoint,
            log_cond,
            x_one,
            x_two,
            y_one,
            y_two,
            survey,
            survey_weight,
        ),
        smem=6,
        scratch=(flat, flat),
        flops=20_000_000,
        limit=6,
        name="forward",
    )

    s_one, s_two = swapped(s_one, s_two, GX)
    t_edge = (size + 2 * rim, rim, depth)
    t_one, t_two = call(pack_seed_kernel, ((t_edge, True),) * 2, (seed, s_one, s_two), name="pack_seed")
    t_one, t_two = swapped(t_one, t_two, GY)
    grad, back = call(
        functools.partial(adjoint_kernel, grid_x, grid_y),
        ((block, False), (block, False)),
        (root, state, later, seed, s_one, s_two, t_one, t_two),
        scratch=(wide, wide, wide, flat, flat, flat),
        flops=20_000_000,
        limit=12,
        name="adjoint",
    )

    near = jnp.sum(from_everyone(partial, ("gx_1", GY)), axis=0)
    total = jnp.sum(from_everyone(near, FAR))
    misfit = (0.5 * total / (grid_x * grid_y * depth)).reshape(1)
    return (grad, back, final, misfit)


def solution(mesh):
    ens, along_x, along_y = (mesh.shape[name] for name in ("ens", "gx", "gy"))
    finer = Mesh(
        mesh.devices.reshape(ens, along_x // 2, 2, along_y), ("ens", "gx_0", "gx_1", "gy")
    )
    field = P(ENS_GX, "gy", None)
    return jax.shard_map(
        on_device,
        mesh=finer,
        in_specs=(field,) * 4 + (P("ens"),) * 6,
        out_specs=(field, field, field, P("ens")),
        check_vma=False,
    )
```

```python
import functools
import math
import operator

import jax
import jax.numpy as jnp
from jax import lax
from jax.experimental import pallas as pl
from jax.experimental.pallas import tpu as pltpu
from jax.sharding import Mesh
from jax.sharding import PartitionSpec as P

FAR = "gx_0"
GX = ("gx_0", "gx_1")
GY = "gy"
ENS_GX = ("ens", "gx_0", "gx_1")

time_step = 0.2
head_slope = 0.5
molecular = 0.05
dispersivity = 0.1

RIM = 2
ROW = 8


def split(value, size):
    if size & (size - 1) == 0:
        return value >> (size.bit_length() - 1), value & (size - 1)
    return lax.div(value, jnp.int32(size)), lax.rem(value, jnp.int32(size))


def place_in(axes):
    position = lax.axis_index(axes)
    return position, position % 2 == 0


def up(field, axis):
    return pltpu.roll(field, field.shape[axis] - 1, axis)


def down(field, axis):
    return pltpu.roll(field, 1, axis)


def lane_mask(shape):
    lane = lax.broadcasted_iota(jnp.int32, shape, 1)
    return jnp.where(lane < shape[1] - 1, jnp.float32(time_step), jnp.float32(0.0))


def row_mask(shape, first, total):
    position = lax.broadcasted_iota(jnp.int32, shape, 0) - ROW + first
    is_open = (position >= 0) & (position + 1 < total)
    return jnp.where(is_open, jnp.float32(time_step), jnp.float32(0.0))


def plane_mask(plane, first, total):
    position = first - RIM + plane
    is_open = (position >= 0) & (position + 1 < total)
    return jnp.where(is_open, jnp.float32(time_step), jnp.float32(0.0))


def visit(count, hit, act):
    group = math.gcd(count, 8)

    def one(base, inner):
        @pl.when(hit(base + inner))
        def _():
            act(base + inner)

    def step(index, carry):
        base = index * group
        anyone = functools.reduce(operator.or_, [hit(base + k) for k in range(group)])

        @pl.when(anyone)
        def _():
            lax.fori_loop(0, group, lambda k, c: (one(base, k), c)[1], 0)

        return carry

    lax.fori_loop(0, count // group, step, 0)


def pack_x_kernel(start_ref, cond_ref, one_ref, two_ref, done):
    size = start_ref.shape[0]
    _, even = place_in(GX)
    first = jnp.where(even, 0, size - RIM)
    second = size - RIM - first
    copies = []
    for out_ref, begin in ((one_ref, first), (two_ref, second)):
        for which, own_ref in ((0, start_ref), (1, cond_ref)):
            source = own_ref.at[pl.ds(begin, RIM)]
            copies.append(
                pltpu.make_async_copy(source, out_ref.at[which], done.at[len(copies)])
            )
    for copy in copies:
        copy.start()
    for copy in copies:
        copy.wait()


def pack_y_kernel(start_ref, cond_ref, x_one_ref, x_two_ref, one_ref, two_ref):
    size, rows = start_ref.shape[:2]
    _, even = place_in(GY)

    def fill(low_ref, high_ref):
        for out_ref, begin in ((low_ref, 0), (high_ref, rows - RIM)):
            span = slice(begin, begin + RIM)
            for which, own_ref in ((0, start_ref), (1, cond_ref)):
                out_ref[which, 0:RIM] = x_one_ref[which, :, span, :]
                out_ref[which, RIM : RIM + size] = own_ref[:, span, :]
                out_ref[which, RIM + size :] = x_two_ref[which, :, span, :]

    @pl.when(even)
    def _():
        fill(one_ref, two_ref)

    @pl.when(jnp.logical_not(even))
    def _():
        fill(two_ref, one_ref)


def pack_seed_kernel(seed_ref, x_one_ref, x_two_ref, one_ref, two_ref):
    size, rows = seed_ref.shape[:2]
    rim = RIM
    _, even = place_in(GY)

    def fill(low_ref, high_ref):
        for out_ref, begin in ((low_ref, 0), (high_ref, rows - rim)):
            span = slice(begin, begin + rim)
            out_ref[0:rim] = x_one_ref[:, span, :]
            out_ref[rim : rim + size] = seed_ref[:, span, :]
            out_ref[rim + size :] = x_two_ref[:, span, :]

    @pl.when(even)
    def _():
        fill(one_ref, two_ref)

    @pl.when(jnp.logical_not(even))
    def _():
        fill(two_ref, one_ref)


def spread(wide_ref, rim, own, x_one, x_two, y_one, y_two):
    size, rows = own.shape
    shift = RIM - rim
    _, even_x = place_in(GX)
    _, even_y = place_in(GY)
    base_one = jnp.where(even_x, shift, RIM + size)
    base_two = shift + RIM + size - base_one

    def copy_own(k, carry):
        wide_ref[RIM + k, ROW : ROW + rows] = own(k)
        return carry

    lax.fori_loop(0, size, copy_own, 0)
    for k in range(rim):
        wide_ref[base_one + k, ROW : ROW + rows] = x_one(k)
        wide_ref[base_two + k, ROW : ROW + rows] = x_two(k)

    def edges(low, high):
        for k in range(size + 2 * rim):
            if k < rim:
                plane = base_one + k
            elif k < rim + size:
                plane = shift + k
            else:
                plane = base_two + k - rim - size
            wide_ref[plane, ROW - rim : ROW] = low(k)
            wide_ref[plane, ROW + rows : ROW + rows + rim] = high(k)

    @pl.when(even_y)
    def _():
        edges(y_one, y_two)

    @pl.when(jnp.logical_not(even_y))
    def _():
        edges(y_two, y_one)


class Own:
    def __init__(self, shape, read):
        self.shape = shape
        self.read = read

    def __call__(self, k):
        return self.read(k)


def forward_kernel(
    grid_x,
    grid_y,
    first_factor,
    second_factor,
    source_cells_ref,
    source_rate_ref,
    well_cells_ref,
    well_data_ref,
    well_weight_ref,
    start_ref,
    cond_ref,
    x_one_ref,
    x_two_ref,
    y_one_ref,
    y_two_ref,
    survey_ref,
    weight_ref,
    root_ref,
    state_ref,
    next_ref,
    final_ref,
    seed_ref,
    edge_one_ref,
    edge_two_ref,
    partial_ref,
    row_ref,
    flux_ref,
    source_cells,
    source_rate,
    well_cells,
    well_data,
    well_weight,
    done,
):
    lists = (
        (source_cells_ref, source_cells),
        (source_rate_ref, source_rate),
        (well_cells_ref, well_cells),
        (well_data_ref, well_data),
        (well_weight_ref, well_weight),
    )
    copies = [
        pltpu.make_async_copy(source, target, done.at[k])
        for k, (source, target) in enumerate(lists)
    ]
    for copy in copies:
        copy.start()
    size, rows, depth = start_ref.shape
    wide = (root_ref.shape[1], depth)
    place_x, even_x = place_in(GX)
    place_y, _ = place_in(GY)
    anchor_x = place_x * size
    anchor_y = place_y * rows

    spread(
        state_ref,
        RIM,
        Own((size, rows), lambda k: start_ref[k]),
        lambda k: x_one_ref[0, k],
        lambda k: x_two_ref[0, k],
        lambda k: y_one_ref[0, k],
        lambda k: y_two_ref[0, k],
    )
    spread(
        root_ref,
        RIM,
        Own((size, rows), lambda k: jnp.exp(0.5 * cond_ref[k])),
        lambda k: jnp.exp(0.5 * x_one_ref[1, k]),
        lambda k: jnp.exp(0.5 * x_two_ref[1, k]),
        lambda k: jnp.exp(0.5 * y_one_ref[1, k]),
        lambda k: jnp.exp(0.5 * y_two_ref[1, k]),
    )
    row_ref[...] = row_mask(wide, anchor_y, grid_y)
    open_z = lane_mask(wide)

    def along_x(ref, plane):
        here = ref[plane]
        ahead = ref[plane + 1]
        cond = root_ref[plane] * root_ref[plane + 1]
        flux = head_slope * cond * here - (molecular + dispersivity * cond) * (ahead - here)
        return flux * plane_mask(plane, anchor_x, grid_x)

    def advanced(ref, plane):
        here = ref[plane]
        root = root_ref[plane]
        flux_x = along_x(ref, plane)
        cond_y = root * up(root, 0)
        flux_y = (row_ref[...] * (molecular + dispersivity * cond_y)) * (here - up(here, 0))
        cond_z = root * up(root, 1)
        flux_z = (open_z * (molecular + dispersivity * cond_z)) * (here - up(here, 1))
        change = (flux_x - flux_ref[...]) + (flux_y - down(flux_y, 0)) + (flux_z - down(flux_z, 1))
        flux_ref[...] = flux_x
        return here - change

    def spot(cell):
        line, along_z = split(cell, depth)
        along_x_, along_y = split(line, grid_y)
        return along_x_ - anchor_x, along_y - anchor_y, along_z

    def within(cell, rim):
        at_x, at_y, _ = spot(cell)
        return (at_x >= -rim) & (at_x < size + rim) & (at_y >= -rim) & (at_y < rows + rim)

    lane = lax.broadcasted_iota(jnp.int32, (1, depth), 1)

    flux_ref[...] = along_x(state_ref, 0)

    def first_step(plane, carry):
        next_ref[plane] = advanced(state_ref, plane)
        return carry

    lax.fori_loop(1, size + 2 * RIM - 1, first_step, 0)

    for copy in copies:
        copy.wait()

    def add_first(index):
        at_x, at_y, at_z = spot(source_cells[index])
        where = (at_x + RIM, pl.ds(at_y + ROW, 1), slice(None))
        amount = time_step * (source_rate[index] * first_factor[0])
        next_ref[where] = next_ref[where] + jnp.where(lane == at_z, amount, 0.0)

    visit(source_cells.shape[0], lambda i: within(source_cells[i], RIM - 1), add_first)

    flux_ref[...] = along_x(next_ref, RIM - 1)

    def second_step(k, carry):
        final_ref[k] = advanced(next_ref, k + RIM)[ROW : ROW + rows]
        return carry

    lax.fori_loop(0, size, second_step, 0)

    def add_second(index):
        at_x, at_y, at_z = spot(source_cells[index])
        where = (at_x, pl.ds(at_y, 1), slice(None))
        amount = time_step * (source_rate[index] * second_factor[0])
        final_ref[where] = final_ref[where] + jnp.where(lane == at_z, amount, 0.0)

    visit(source_cells.shape[0], lambda i: within(source_cells[i], 0), add_second)

    partial_ref[...] = jnp.zeros((1, depth), jnp.float32)

    def compare(k, total):
        missed = final_ref[k] - survey_ref[k]
        seed = weight_ref[k] * missed
        seed_ref[k] = seed
        return total + jnp.sum((seed * missed).reshape(rows // 8, 8, depth), axis=0)

    total = lax.fori_loop(0, size, compare, jnp.zeros((8, depth), jnp.float32))
    partial_ref[...] = jnp.sum(total, axis=0, keepdims=True)

    def observe(index):
        at_x, at_y, at_z = spot(well_cells[index])
        where = (at_x, pl.ds(at_y, 1), slice(None))
        nearby = final_ref[where] - well_data[index]
        pull = jnp.where(lane == at_z, well_weight[index] * nearby, 0.0)
        seed_ref[where] = seed_ref[where] + pull
        partial_ref[...] = partial_ref[...] + pull * nearby

    visit(well_cells.shape[0], lambda i: within(well_cells[i], 0), observe)

    first = jnp.where(even_x, 0, size - RIM)
    second = size - RIM - first
    for k in range(RIM):
        edge_one_ref[k] = seed_ref[first + k]
        edge_two_ref[k] = seed_ref[second + k]


def adjoint_kernel(
    grid_x,
    grid_y,
    root_ref,
    state_ref,
    next_ref,
    seed_ref,
    x_one_ref,
    x_two_ref,
    y_one_ref,
    y_two_ref,
    grad_ref,
    back_ref,
    last_ref,
    middle_ref,
    partial_ref,
    row_ref,
    pull_ref,
    sens_ref,
):
    size, rows, depth = seed_ref.shape
    wide = (root_ref.shape[1], depth)
    place_x, _ = place_in(GX)
    place_y, _ = place_in(GY)
    anchor_x = place_x * size
    anchor_y = place_y * rows
    spread(
        last_ref,
        RIM,
        Own((size, rows), lambda k: seed_ref[k]),
        lambda k: x_one_ref[k],
        lambda k: x_two_ref[k],
        lambda k: y_one_ref[k],
        lambda k: y_two_ref[k],
    )
    row_ref[...] = row_mask(wide, anchor_y, grid_y)
    open_z = lane_mask(wide)

    def along_x(adjoint_ref, tracer_ref, plane):
        jump = plane_mask(plane, anchor_x, grid_x) * (adjoint_ref[plane + 1] - adjoint_ref[plane])
        cond = root_ref[plane] * root_ref[plane + 1]
        pull = jump * (molecular + dispersivity * cond)
        push = jump * (head_slope * cond) + pull
        here = tracer_ref[plane]
        rise = head_slope * here - dispersivity * (tracer_ref[plane + 1] - here)
        return push, pull, jump * rise * (0.5 * cond)

    def along(adjoint, tracer, root, is_open, axis):
        jump = is_open * (up(adjoint, axis) - adjoint)
        cond = root * up(root, axis)
        pull = jump * (molecular + dispersivity * cond)
        sens = (jump * (tracer - up(tracer, axis))) * ((0.5 * dispersivity) * cond)
        return pull - down(pull, axis), sens + down(sens, axis)

    def reversed_step(adjoint_ref, tracer_ref, plane):
        push, pull, sens = along_x(adjoint_ref, tracer_ref, plane)
        adjoint = adjoint_ref[plane]
        tracer = tracer_ref[plane]
        root = root_ref[plane]
        change_y, sens_y = along(adjoint, tracer, root, row_ref[...], 0)
        change_z, sens_z = along(adjoint, tracer, root, open_z, 1)
        updated = adjoint + (push - pull_ref[...]) + change_y + change_z
        gradient = (sens + sens_ref[...]) + sens_y + sens_z
        pull_ref[...] = pull
        sens_ref[...] = sens
        return updated, gradient

    def begin(adjoint_ref, tracer_ref, plane):
        _, pull, sens = along_x(adjoint_ref, tracer_ref, plane)
        pull_ref[...] = pull
        sens_ref[...] = sens

    begin(last_ref, next_ref, RIM - 2)

    def later(plane, carry):
        updated, gradient = reversed_step(last_ref, next_ref, plane)
        middle_ref[plane] = updated
        partial_ref[plane] = gradient
        return carry

    lax.fori_loop(RIM - 1, size + RIM + 1, later, 0)

    begin(middle_ref, state_ref, RIM - 1)

    def earlier(k, carry):
        updated, gradient = reversed_step(middle_ref, state_ref, k + RIM)
        back_ref[k] = updated[ROW : ROW + rows]
        grad_ref[k] = (gradient + partial_ref[k + RIM])[ROW : ROW + rows]
        return carry

    lax.fori_loop(0, size, earlier, 0)


def call(kernel, outs, operands, *, scratch=(), flops=1_000_000, limit=2):
    shapes = tuple(
        jax.ShapeDtypeStruct(shape, jnp.float32) if space is None else space(shape, jnp.float32)
        for shape, space in outs
    )
    arrays = [
        array if space == pltpu.SMEM else pltpu.with_memory_space_constraint(array, space)
        for array, space in operands
    ]
    return pl.pallas_call(
        kernel,
        out_shape=shapes,
        in_specs=[pl.BlockSpec(memory_space=space) for _, space in operands],
        out_specs=tuple(pl.BlockSpec(memory_space=pltpu.VMEM) for _ in outs),
        scratch_shapes=scratch,
        cost_estimate=pl.CostEstimate(flops=flops, transcendentals=0, bytes_accessed=1_000_000),
        compiler_params=pltpu.CompilerParams(vmem_limit_bytes=limit << 20),
    )(*arrays)


def kept(*arrays, space=pltpu.VMEM):
    return tuple((array, space) for array in arrays)


def swapped(one, two, axes):
    count = lax.axis_size(axes)
    outer = [(i, i + 1) for i in range(1, count - 1, 2)]
    inner = [(i, i + 1) for i in range(0, count - 1, 2)]
    back = lambda pairs: pairs + [(b, a) for a, b in pairs]
    return lax.ppermute(one, axes, back(outer)), lax.ppermute(two, axes, back(inner))


def from_everyone(shard, axis):
    count = lax.axis_size(axis)
    return lax.all_to_all(
        jnp.broadcast_to(shard[None], (count, *shard.shape)), axis, 0, 0, tiled=True
    )


def on_device(
    log_cond,
    checkpoint,
    survey,
    survey_weight,
    well_cells,
    well_data,
    well_weight,
    source_cells,
    source_rate,
    step_number,
):
    size, rows, depth = checkpoint.shape
    grid_x = size * lax.axis_size(GX)
    grid_y = rows * lax.axis_size(GY)
    clock = step_number.astype(jnp.float32)
    first_factor = 1.0 + 0.5 * jnp.sin(0.05 * clock)
    second_factor = 1.0 + 0.5 * jnp.sin(0.05 * (clock + 1.0))

    planes = size + 2 * RIM
    wide = (planes, rows + 2 * ROW, depth)
    flat = wide[1:]
    block = (size, rows, depth)
    f32 = functools.partial(pltpu.VMEM, dtype=jnp.float32)
    dma = pltpu.SemaphoreType.DMA

    x_edge = (2, RIM, rows, depth)
    x_one, x_two = call(
        pack_x_kernel,
        kept(x_edge, x_edge),
        kept(checkpoint, log_cond, space=pltpu.HBM),
        scratch=[dma((4,))],
    )
    x_one, x_two = swapped(x_one, x_two, GX)
    y_edge = (2, planes, RIM, depth)
    y_one, y_two = call(
        pack_y_kernel, kept(y_edge, y_edge), kept(checkpoint, log_cond, x_one, x_two)
    )
    y_one, y_two = swapped(y_one, y_two, GY)

    s_edge = (RIM, rows, depth)
    lists = (source_cells, source_rate, well_cells, well_data, well_weight)
    fields = (checkpoint, log_cond, x_one, x_two, y_one, y_two, survey, survey_weight)
    root, state, later, final, seed, s_one, s_two, partial = call(
        functools.partial(forward_kernel, grid_x, grid_y),
        kept(wide, wide, wide)
        + kept(block, space=None)
        + kept(block, s_edge, s_edge, (1, depth)),
        kept(first_factor, second_factor, space=pltpu.SMEM)
        + kept(*lists, space=pltpu.HBM)
        + kept(*fields),
        scratch=[f32(flat), f32(flat)]
        + [pltpu.SMEM(array.shape, array.dtype) for array in lists]
        + [dma((len(lists),))],
        flops=20_000_000,
        limit=4,
    )

    s_one, s_two = swapped(s_one, s_two, GX)
    t_edge = (planes, RIM, depth)
    t_one, t_two = call(pack_seed_kernel, kept(t_edge, t_edge), kept(seed, s_one, s_two))
    t_one, t_two = swapped(t_one, t_two, GY)
    grad, back = call(
        functools.partial(adjoint_kernel, grid_x, grid_y),
        kept(block, block, space=None),
        kept(root, state, later, seed, s_one, s_two, t_one, t_two),
        scratch=[f32(wide)] * 3 + [f32(flat)] * 3,
        flops=20_000_000,
        limit=6,
    )

    near = jnp.sum(from_everyone(partial, ("gx_1", GY)), axis=0)
    everyone = from_everyone(near, FAR)
    misfit = (0.5 * jnp.sum(everyone) / (grid_x * grid_y * depth)).reshape(1)
    return (grad, back, final, misfit)


def solution(mesh):
    ens, along_x, along_y = (mesh.shape[name] for name in ("ens", "gx", "gy"))
    finer = Mesh(
        mesh.devices.reshape(ens, along_x // 2, 2, along_y), ("ens", "gx_0", "gx_1", "gy")
    )
    field = P(ENS_GX, "gy", None)

    return jax.shard_map(
        on_device,
        mesh=finer,
        in_specs=(field,) * 4 + (P("ens"),) * 6,
        out_specs=(field, field, field, P("ens")),
        check_vma=False,
    )
```

```python
import functools
import math
import operator

import jax
import jax.numpy as jnp
from jax import lax
from jax.experimental import pallas as pl
from jax.experimental.pallas import tpu as pltpu
from jax.sharding import Mesh
from jax.sharding import PartitionSpec as P

FAR = "gx_0"
GX = ("gx_0", "gx_1")
GY = "gy"
ENS_GX = ("ens", "gx_0", "gx_1")

time_step = 0.2
head_slope = 0.5
molecular = 0.05
dispersivity = 0.1

RIM = 2
ROW = 8
LINES = 1024
PAD = 8


def split(value, size):
    if size & (size - 1) == 0:
        return value >> (size.bit_length() - 1), value & (size - 1)
    return lax.div(value, jnp.int32(size)), lax.rem(value, jnp.int32(size))


def place_in(axes):
    position = lax.axis_index(axes)
    return position, position % 2 == 0


def up(field, axis):
    return pltpu.roll(field, field.shape[axis] - 1, axis)


def down(field, axis):
    return pltpu.roll(field, 1, axis)


def lane_mask(shape):
    lane = lax.broadcasted_iota(jnp.int32, shape, 1)
    return jnp.where(lane < shape[1] - 1, jnp.float32(time_step), jnp.float32(0.0))


def row_mask(shape, first, total):
    position = lax.broadcasted_iota(jnp.int32, shape, 0) - ROW + first
    is_open = (position >= 0) & (position + 1 < total)
    return jnp.where(is_open, jnp.float32(time_step), jnp.float32(0.0))


def plane_mask(plane, first, total):
    position = first - RIM + plane
    is_open = (position >= 0) & (position + 1 < total)
    return jnp.where(is_open, jnp.float32(time_step), jnp.float32(0.0))


def visit(count, outside, act):
    group = math.gcd(count, 8)

    def one(index):
        @pl.when(outside(index) >= 0)
        def _():
            act(index)

    def step(number, carry):
        base = number * group
        everyone = functools.reduce(operator.and_, [outside(base + k) for k in range(group)])

        @pl.when(everyone >= 0)
        def _():
            lax.fori_loop(0, group, lambda k, c: (one(base + k), c)[1], 0)

        return carry

    lax.fori_loop(0, count // group, step, 0)


def start_copies(sources, targets, done):
    copies = [
        pltpu.make_async_copy(source, target, done.at[k])
        for k, (source, target) in enumerate(zip(sources, targets))
    ]
    for copy in copies:
        copy.start()
    return copies


def pack_x_kernel(start_ref, cond_ref, one_ref, two_ref, done):
    size = start_ref.shape[0]
    _, even = place_in(GX)
    first = jnp.where(even, 0, size - RIM)
    second = size - RIM - first
    copies = []
    for out_ref, begin in ((one_ref, first), (two_ref, second)):
        for which, own_ref in ((0, start_ref), (1, cond_ref)):
            source = own_ref.at[pl.ds(begin, RIM)]
            copies.append(
                pltpu.make_async_copy(source, out_ref.at[which], done.at[len(copies)])
            )
    for copy in copies:
        copy.start()
    for copy in copies:
        copy.wait()


def pack_y_kernel(start_ref, cond_ref, x_one_ref, x_two_ref, one_ref, two_ref):
    size, rows = start_ref.shape[:2]
    _, even = place_in(GY)

    def fill(low_ref, high_ref):
        for out_ref, begin in ((low_ref, 0), (high_ref, rows - RIM)):
            span = slice(begin, begin + RIM)
            for which, own_ref in ((0, start_ref), (1, cond_ref)):
                out_ref[which, 0:RIM] = x_one_ref[which, :, span, :]
                out_ref[which, RIM : RIM + size] = own_ref[:, span, :]
                out_ref[which, RIM + size :] = x_two_ref[which, :, span, :]

    @pl.when(even)
    def _():
        fill(one_ref, two_ref)

    @pl.when(jnp.logical_not(even))
    def _():
        fill(two_ref, one_ref)


def pack_seed_kernel(seed_ref, x_one_ref, x_two_ref, one_ref, two_ref):
    size, rows = seed_ref.shape[:2]
    rim = RIM
    _, even = place_in(GY)

    def fill(low_ref, high_ref):
        for out_ref, begin in ((low_ref, 0), (high_ref, rows - rim)):
            span = slice(begin, begin + rim)
            out_ref[0:rim] = x_one_ref[:, span, :]
            out_ref[rim : rim + size] = seed_ref[:, span, :]
            out_ref[rim + size :] = x_two_ref[:, span, :]

    @pl.when(even)
    def _():
        fill(one_ref, two_ref)

    @pl.when(jnp.logical_not(even))
    def _():
        fill(two_ref, one_ref)


def spread(wide_ref, rim, own, x_one, x_two, y_one, y_two):
    size, rows = own.shape
    shift = RIM - rim
    _, even_x = place_in(GX)
    _, even_y = place_in(GY)
    base_one = jnp.where(even_x, shift, RIM + size)
    base_two = shift + RIM + size - base_one


    def copy_own(k, carry):
        wide_ref[RIM + k, ROW : ROW + rows] = own.read(k)
        return carry

    lax.fori_loop(0, size, copy_own, 0)
    for k in range(rim):
        wide_ref[base_one + k, ROW : ROW + rows] = x_one(k)
        wide_ref[base_two + k, ROW : ROW + rows] = x_two(k)

    def edges(low, high):
        for k in range(size + 2 * rim):
            if k < rim:
                plane = base_one + k
            elif k < rim + size:
                plane = shift + k
            else:
                plane = base_two + k - rim - size
            wide_ref[plane, ROW - rim : ROW] = low(k)
            wide_ref[plane, ROW + rows : ROW + rows + rim] = high(k)

    @pl.when(even_y)
    def _():
        edges(y_one, y_two)

    @pl.when(jnp.logical_not(even_y))
    def _():
        edges(y_two, y_one)


class Own:
    def __init__(self, shape, read):
        self.shape = shape
        self.read = read


def pack_spot(at_x, at_y, at_z, depth):
    return ((at_x + RIM) * LINES + at_y + ROW) * depth + at_z


def unpack_spot(code, depth):
    line, at_z = split(code, depth)
    plane, row = split(line, LINES)
    return plane, row, at_z


def lay_kernel(
    grid_y,
    first_factor,
    second_factor,
    source_cells_ref,
    source_rate_ref,
    well_cells_ref,
    well_data_ref,
    well_weight_ref,
    cond_ref,
    root_ref,
    source_spot,
    first_amount,
    second_amount,
    well_spot,
    well_level,
    well_pull,
    source_cells,
    source_rate,
    well_cells,
    well_data,
    well_weight,
    done,
):
    copies = start_copies(
        (source_cells_ref, source_rate_ref, well_cells_ref, well_data_ref, well_weight_ref),
        (source_cells, source_rate, well_cells, well_data, well_weight),
        done,
    )
    size, rows, depth = cond_ref.shape
    place_x, _ = place_in(GX)
    place_y, _ = place_in(GY)
    anchor_x = place_x * size
    anchor_y = place_y * rows
    sources = source_cells.shape[0]
    wells = well_cells.shape[0]

    def own(k, carry):
        root_ref[k] = jnp.exp(0.5 * cond_ref[k])
        return carry

    lax.fori_loop(0, size, own, 0)
    for copy in copies:
        copy.wait()

    def spot(cell):
        line, at_z = split(cell, depth)
        at_x, at_y = split(line, grid_y)
        return at_x - anchor_x, at_y - anchor_y, at_z

    def outside(cell, rim):
        at_x, at_y, _ = spot(cell)
        return (
            (at_x + rim) | (size - 1 + rim - at_x) | (at_y + rim) | (rows - 1 + rim - at_y)
        )

    source_spot[sources] = 0
    well_spot[wells] = 0

    def add_source(index):
        slot = source_spot[sources]
        source_spot[slot] = pack_spot(*spot(source_cells[index]), depth)
        first_amount[slot] = time_step * (source_rate[index] * first_factor[0])
        second_amount[slot] = time_step * (source_rate[index] * second_factor[0])
        source_spot[sources] = slot + 1

    visit(sources, lambda i: outside(source_cells[i], RIM - 1), add_source)

    def add_well(index):
        slot = well_spot[wells]
        well_spot[slot] = pack_spot(*spot(well_cells[index]), depth)
        well_level[slot] = well_data[index]
        well_pull[slot] = well_weight[index]
        well_spot[wells] = slot + 1

    visit(wells, lambda i: outside(well_cells[i], 0), add_well)


def sum_kernel(shares_ref, out_ref):
    total = jnp.sum(shares_ref[...], axis=0)
    for k in range(out_ref.shape[0]):
        out_ref[k] = total


def forward_kernel(
    grid_x,
    grid_y,
    source_spot_ref,
    first_amount_ref,
    second_amount_ref,
    well_spot_ref,
    well_level_ref,
    well_pull_ref,
    own_root_ref,
    start_ref,
    x_one_ref,
    x_two_ref,
    y_one_ref,
    y_two_ref,
    survey_ref,
    weight_ref,
    root_ref,
    state_ref,
    next_ref,
    final_ref,
    seed_ref,
    edge_one_ref,
    edge_two_ref,
    partial_ref,
    row_ref,
    flux_ref,
    source_spot,
    first_amount,
    second_amount,
    well_spot,
    well_level,
    well_pull,
    done,
):
    copies = start_copies(
        (
            source_spot_ref,
            first_amount_ref,
            second_amount_ref,
            well_spot_ref,
            well_level_ref,
            well_pull_ref,
        ),
        (source_spot, first_amount, second_amount, well_spot, well_level, well_pull),
        done,
    )
    size, rows, depth = survey_ref.shape
    wide = (root_ref.shape[1], depth)
    place_x, even_x = place_in(GX)
    place_y, _ = place_in(GY)
    anchor_x = place_x * size
    anchor_y = place_y * rows

    spread(
        state_ref,
        RIM,
        Own((size, rows), lambda k: start_ref[k]),
        lambda k: x_one_ref[0, k],
        lambda k: x_two_ref[0, k],
        lambda k: y_one_ref[0, k],
        lambda k: y_two_ref[0, k],
    )
    spread(
        root_ref,
        RIM,
        Own((size, rows), lambda k: own_root_ref[k]),
        lambda k: jnp.exp(0.5 * x_one_ref[1, k]),
        lambda k: jnp.exp(0.5 * x_two_ref[1, k]),
        lambda k: jnp.exp(0.5 * y_one_ref[1, k]),
        lambda k: jnp.exp(0.5 * y_two_ref[1, k]),
    )
    row_ref[...] = row_mask(wide, anchor_y, grid_y)
    open_z = lane_mask(wide)

    def along_x(ref, plane):
        here = ref[plane]
        ahead = ref[plane + 1]
        cond = root_ref[plane] * root_ref[plane + 1]
        flux = head_slope * cond * here - (molecular + dispersivity * cond) * (ahead - here)
        return flux * plane_mask(plane, anchor_x, grid_x)

    def advanced(ref, plane):
        here = ref[plane]
        root = root_ref[plane]
        flux_x = along_x(ref, plane)
        cond_y = root * up(root, 0)
        flux_y = (row_ref[...] * (molecular + dispersivity * cond_y)) * (here - up(here, 0))
        cond_z = root * up(root, 1)
        flux_z = (open_z * (molecular + dispersivity * cond_z)) * (here - up(here, 1))
        change = (flux_x - flux_ref[...]) + (flux_y - down(flux_y, 0)) + (flux_z - down(flux_z, 1))
        flux_ref[...] = flux_x
        return here - change

    lane = lax.broadcasted_iota(jnp.int32, (1, depth), 1)

    flux_ref[...] = along_x(state_ref, 0)

    def first_step(plane, carry):
        next_ref[plane] = advanced(state_ref, plane)
        return carry

    lax.fori_loop(1, size + 2 * RIM - 1, first_step, 0)

    for copy in copies:
        copy.wait()

    sources = source_spot[source_spot.shape[0] - PAD]

    def add_first(index, carry):
        plane, row, at_z = unpack_spot(source_spot[index], depth)
        where = (plane, pl.ds(row, 1), slice(None))
        next_ref[where] = next_ref[where] + jnp.where(lane == at_z, first_amount[index], 0.0)
        return carry

    lax.fori_loop(0, sources, add_first, 0)

    flux_ref[...] = along_x(next_ref, RIM - 1)

    def second_step(k, carry):
        final_ref[k] = advanced(next_ref, k + RIM)[ROW : ROW + rows]
        return carry

    lax.fori_loop(0, size, second_step, 0)

    def add_second(index, carry):
        plane, row, at_z = unpack_spot(source_spot[index], depth)
        plane = plane - RIM
        row = row - ROW

        @pl.when((plane >= 0) & (plane < size) & (row >= 0) & (row < rows))
        def _():
            where = (plane, pl.ds(row, 1), slice(None))
            amount = second_amount[index]
            final_ref[where] = final_ref[where] + jnp.where(lane == at_z, amount, 0.0)

        return carry

    lax.fori_loop(0, sources, add_second, 0)

    def compare(k, total):
        missed = final_ref[k] - survey_ref[k]
        seed = weight_ref[k] * missed
        seed_ref[k] = seed
        return total + jnp.sum((seed * missed).reshape(rows // 8, 8, depth), axis=0)

    total = lax.fori_loop(0, size, compare, jnp.zeros((8, depth), jnp.float32))

    def observe(index, total):
        plane, row, at_z = unpack_spot(well_spot[index], depth)
        where = (plane - RIM, pl.ds(row - ROW, 1), slice(None))
        nearby = final_ref[where] - well_level[index]
        pull = jnp.where(lane == at_z, well_pull[index] * nearby, 0.0)
        seed_ref[where] = seed_ref[where] + pull
        return total + pull * nearby

    wells = well_spot[well_spot.shape[0] - PAD]
    total = lax.fori_loop(0, wells, observe, jnp.sum(total, axis=0, keepdims=True))
    total = total * (0.5 / (grid_x * grid_y * depth))
    for k in range(partial_ref.shape[0]):
        partial_ref[k] = total

    first = jnp.where(even_x, 0, size - RIM)
    second = size - RIM - first
    for k in range(RIM):
        edge_one_ref[k] = seed_ref[first + k]
        edge_two_ref[k] = seed_ref[second + k]


def adjoint_kernel(
    grid_x,
    grid_y,
    root_ref,
    state_ref,
    next_ref,
    seed_ref,
    x_one_ref,
    x_two_ref,
    y_one_ref,
    y_two_ref,
    grad_ref,
    back_ref,
    last_ref,
    middle_ref,
    partial_ref,
    row_ref,
    pull_ref,
    sens_ref,
):
    size, rows, depth = seed_ref.shape
    wide = (root_ref.shape[1], depth)
    place_x, _ = place_in(GX)
    place_y, _ = place_in(GY)
    anchor_x = place_x * size
    anchor_y = place_y * rows
    spread(
        last_ref,
        RIM,
        Own((size, rows), lambda k: seed_ref[k]),
        lambda k: x_one_ref[k],
        lambda k: x_two_ref[k],
        lambda k: y_one_ref[k],
        lambda k: y_two_ref[k],
    )
    row_ref[...] = row_mask(wide, anchor_y, grid_y)
    open_z = lane_mask(wide)

    def along_x(adjoint_ref, tracer_ref, plane):
        jump = plane_mask(plane, anchor_x, grid_x) * (adjoint_ref[plane + 1] - adjoint_ref[plane])
        cond = root_ref[plane] * root_ref[plane + 1]
        pull = jump * (molecular + dispersivity * cond)
        push = jump * (head_slope * cond) + pull
        here = tracer_ref[plane]
        rise = head_slope * here - dispersivity * (tracer_ref[plane + 1] - here)
        return push, pull, jump * rise * (0.5 * cond)

    def along(adjoint, tracer, root, is_open, axis):
        jump = is_open * (up(adjoint, axis) - adjoint)
        cond = root * up(root, axis)
        pull = jump * (molecular + dispersivity * cond)
        sens = (jump * (tracer - up(tracer, axis))) * ((0.5 * dispersivity) * cond)
        return pull - down(pull, axis), sens + down(sens, axis)

    def reversed_step(adjoint_ref, tracer_ref, plane):
        push, pull, sens = along_x(adjoint_ref, tracer_ref, plane)
        adjoint = adjoint_ref[plane]
        tracer = tracer_ref[plane]
        root = root_ref[plane]
        change_y, sens_y = along(adjoint, tracer, root, row_ref[...], 0)
        change_z, sens_z = along(adjoint, tracer, root, open_z, 1)
        updated = adjoint + (push - pull_ref[...]) + change_y + change_z
        gradient = (sens + sens_ref[...]) + sens_y + sens_z
        pull_ref[...] = pull
        sens_ref[...] = sens
        return updated, gradient

    def begin(adjoint_ref, tracer_ref, plane):
        _, pull, sens = along_x(adjoint_ref, tracer_ref, plane)
        pull_ref[...] = pull
        sens_ref[...] = sens

    begin(last_ref, next_ref, RIM - 2)

    def later(plane, carry):
        updated, gradient = reversed_step(last_ref, next_ref, plane)
        middle_ref[plane] = updated
        partial_ref[plane] = gradient
        return carry

    lax.fori_loop(RIM - 1, size + RIM + 1, later, 0)

    begin(middle_ref, state_ref, RIM - 1)

    def earlier(k, carry):
        updated, gradient = reversed_step(middle_ref, state_ref, k + RIM)
        back_ref[k] = updated[ROW : ROW + rows]
        grad_ref[k] = (gradient + partial_ref[k + RIM])[ROW : ROW + rows]
        return carry

    lax.fori_loop(0, size, earlier, 0)


def call(kernel, outs, operands, *, scratch=(), flops=1_000_000, limit=2):
    shapes = tuple(
        space(shape, jnp.float32)
        if space == pltpu.VMEM
        else jax.ShapeDtypeStruct(*shape)
        if space == pltpu.SMEM
        else jax.ShapeDtypeStruct(shape, jnp.float32)
        for shape, space in outs
    )
    arrays = [
        array if space == pltpu.SMEM else pltpu.with_memory_space_constraint(array, space)
        for array, space in operands
    ]
    out_spaces = [pltpu.VMEM if space is None else space for _, space in outs]
    return pl.pallas_call(
        kernel,
        out_shape=shapes,
        in_specs=[pl.BlockSpec(memory_space=space) for _, space in operands],
        out_specs=tuple(pl.BlockSpec(memory_space=space) for space in out_spaces),
        scratch_shapes=scratch,
        cost_estimate=pl.CostEstimate(flops=flops, transcendentals=0, bytes_accessed=1_000_000),
        compiler_params=pltpu.CompilerParams(vmem_limit_bytes=limit << 20),
    )(*arrays)


def kept(*arrays, space=pltpu.VMEM):
    return tuple((array, space) for array in arrays)


def swapped(one, two, axes):
    count = lax.axis_size(axes)
    outer = [(i, i + 1) for i in range(1, count - 1, 2)]
    inner = [(i, i + 1) for i in range(0, count - 1, 2)]
    back = lambda pairs: pairs + [(b, a) for a, b in pairs]
    one = lax.ppermute(one, axes, back(outer))
    two = lax.ppermute(two, axes, back(inner))
    return one, two


def on_device(
    log_cond,
    checkpoint,
    survey,
    survey_weight,
    well_cells,
    well_data,
    well_weight,
    source_cells,
    source_rate,
    step_number,
):
    size, rows, depth = checkpoint.shape
    grid_x = size * lax.axis_size(GX)
    grid_y = rows * lax.axis_size(GY)
    clock = step_number.astype(jnp.float32)
    first_factor = 1.0 + 0.5 * jnp.sin(0.05 * clock)
    second_factor = 1.0 + 0.5 * jnp.sin(0.05 * (clock + 1.0))

    planes = size + 2 * RIM
    wide = (planes, rows + 2 * ROW, depth)
    flat = wide[1:]
    block = (size, rows, depth)
    f32 = functools.partial(pltpu.VMEM, dtype=jnp.float32)
    dma = pltpu.SemaphoreType.DMA

    x_edge = (2, RIM, rows, depth)
    x_one, x_two = call(
        pack_x_kernel,
        kept(x_edge, x_edge),
        kept(checkpoint, log_cond, space=pltpu.HBM),
        scratch=[dma((4,))],
    )
    x_one, x_two = swapped(x_one, x_two, GX)

    lists = (source_cells, source_rate, well_cells, well_data, well_weight)
    sources = source_cells.shape[0] + PAD
    wells = well_cells.shape[0] + PAD
    found = (
        ((sources,), jnp.int32),
        ((sources,), jnp.float32),
        ((sources,), jnp.float32),
        ((wells,), jnp.int32),
        ((wells,), jnp.float32),
        ((wells,), jnp.float32),
    )
    root, *hits = call(
        functools.partial(lay_kernel, grid_y),
        kept(block) + kept(*found, space=pltpu.SMEM),
        kept(first_factor, second_factor, space=pltpu.SMEM)
        + kept(*lists, space=pltpu.HBM)
        + kept(log_cond),
        scratch=[pltpu.SMEM(array.shape, array.dtype) for array in lists]
        + [dma((len(lists),))],
        flops=4_000_000,
    )

    y_edge = (2, planes, RIM, depth)
    y_one, y_two = call(
        pack_y_kernel, kept(y_edge, y_edge), kept(checkpoint, log_cond, x_one, x_two)
    )
    y_one, y_two = swapped(y_one, y_two, GY)

    s_edge = (RIM, rows, depth)
    near_axes = ("gx_1", GY)
    near_count = lax.axis_size(near_axes)
    fields = (root, checkpoint, x_one, x_two, y_one, y_two, survey, survey_weight)
    root, state, later, final, seed, s_one, s_two, partial = call(
        functools.partial(forward_kernel, grid_x, grid_y),
        kept(wide, wide, wide)
        + kept(block, space=None)
        + kept(block, s_edge, s_edge, (near_count, 1, depth)),
        kept(*hits, space=pltpu.HBM) + kept(*fields),
        scratch=[f32(flat), f32(flat)]
        + [pltpu.SMEM(array.shape, array.dtype) for array in hits]
        + [dma((len(hits),))],
        flops=20_000_000,
        limit=4,
    )

    near = lax.all_to_all(partial, near_axes, 0, 0, tiled=True)
    (near,) = call(sum_kernel, kept((lax.axis_size(FAR), 1, depth)), kept(near))
    everyone = lax.all_to_all(near, FAR, 0, 0, tiled=True)
    misfit = jnp.sum(everyone).reshape(1)

    s_one, s_two = swapped(s_one, s_two, GX)
    t_edge = (planes, RIM, depth)
    t_one, t_two = call(pack_seed_kernel, kept(t_edge, t_edge), kept(seed, s_one, s_two))
    t_one, t_two = swapped(t_one, t_two, GY)
    grad, back = call(
        functools.partial(adjoint_kernel, grid_x, grid_y),
        kept(block, block, space=None),
        kept(root, state, later, seed, s_one, s_two, t_one, t_two),
        scratch=[f32(wide)] * 3 + [f32(flat)] * 3,
        flops=20_000_000,
        limit=6,
    )
    return (grad, back, final, misfit)


def solution(mesh):
    ens, along_x, along_y = (mesh.shape[name] for name in ("ens", "gx", "gy"))
    finer = Mesh(
        mesh.devices.reshape(ens, along_x // 2, 2, along_y), ("ens", "gx_0", "gx_1", "gy")
    )
    field = P(ENS_GX, "gy", None)

    return jax.shard_map(
        on_device,
        mesh=finer,
        in_specs=(field,) * 4 + (P("ens"),) * 6,
        out_specs=(field, field, field, P("ens")),
        check_vma=False,
    )
```

```python
import functools
import math
import operator

import jax
import jax.numpy as jnp
from jax import lax
from jax.experimental import pallas as pl
from jax.experimental.pallas import tpu as pltpu
from jax.sharding import Mesh
from jax.sharding import PartitionSpec as P

FAR = "gx_0"
GX = ("gx_0", "gx_1")
GY = "gy"
ENS_GX = ("ens", "gx_0", "gx_1")

time_step = 0.2
head_slope = 0.5
molecular = 0.05
dispersivity = 0.1

RIM = 2
ROW = 8
LINES = 1024
PAD = 8


def split(value, size):
    if size & (size - 1) == 0:
        return value >> (size.bit_length() - 1), value & (size - 1)
    return lax.div(value, jnp.int32(size)), lax.rem(value, jnp.int32(size))


def place_in(axes):
    position = lax.axis_index(axes)
    return position, position % 2 == 0


def up(field, axis):
    return pltpu.roll(field, field.shape[axis] - 1, axis)


def down(field, axis):
    return pltpu.roll(field, 1, axis)


def lane_mask(shape):
    lane = lax.broadcasted_iota(jnp.int32, shape, 1)
    return jnp.where(lane < shape[1] - 1, jnp.float32(time_step), jnp.float32(0.0))


def row_mask(shape, first, total):
    position = lax.broadcasted_iota(jnp.int32, shape, 0) - ROW + first
    is_open = (position >= 0) & (position + 1 < total)
    return jnp.where(is_open, jnp.float32(time_step), jnp.float32(0.0))


def plane_mask(plane, first, total):
    position = first - RIM + plane
    is_open = (position >= 0) & (position + 1 < total)
    return jnp.where(is_open, jnp.float32(time_step), jnp.float32(0.0))


def visit(count, outside, check, act):
    group = math.gcd(count, 8)

    def one(index):
        @pl.when(outside(index) >= 0)
        def _():
            @pl.when(check(index))
            def _():
                act(index)

    def step(number, carry):
        base = number * group
        everyone = functools.reduce(operator.and_, [outside(base + k) for k in range(group)])

        @pl.when(everyone >= 0)
        def _():
            lax.fori_loop(0, group, lambda k, c: (one(base + k), c)[1], 0)

        return carry

    lax.fori_loop(0, count // group, step, 0)


def start_copies(sources, targets, done):
    copies = [
        pltpu.make_async_copy(source, target, done.at[k])
        for k, (source, target) in enumerate(zip(sources, targets))
    ]
    for copy in copies:
        copy.start()
    return copies


def pack_x_kernel(start_ref, cond_ref, one_ref, two_ref, done):
    size = start_ref.shape[0]
    _, even = place_in(GX)
    first = jnp.where(even, 0, size - RIM)
    second = size - RIM - first
    copies = []
    for out_ref, begin in ((one_ref, first), (two_ref, second)):
        for which, own_ref in ((0, start_ref), (1, cond_ref)):
            source = own_ref.at[pl.ds(begin, RIM)]
            copies.append(
                pltpu.make_async_copy(source, out_ref.at[which], done.at[len(copies)])
            )
    for copy in copies:
        copy.start()
    for copy in copies:
        copy.wait()


def pack_y_kernel(start_ref, cond_ref, x_one_ref, x_two_ref, one_ref, two_ref):
    size, rows = start_ref.shape[:2]
    _, even = place_in(GY)

    def fill(low_ref, high_ref):
        for out_ref, begin in ((low_ref, 0), (high_ref, rows - RIM)):
            span = slice(begin, begin + RIM)
            for which, own_ref in ((0, start_ref), (1, cond_ref)):
                out_ref[which, 0:RIM] = x_one_ref[which, :, span, :]
                out_ref[which, RIM : RIM + size] = own_ref[:, span, :]
                out_ref[which, RIM + size :] = x_two_ref[which, :, span, :]

    @pl.when(even)
    def _():
        fill(one_ref, two_ref)

    @pl.when(jnp.logical_not(even))
    def _():
        fill(two_ref, one_ref)


def pack_seed_kernel(seed_ref, x_one_ref, x_two_ref, one_ref, two_ref):
    size, rows = seed_ref.shape[:2]
    rim = RIM
    _, even = place_in(GY)

    def fill(low_ref, high_ref):
        for out_ref, begin in ((low_ref, 0), (high_ref, rows - rim)):
            span = slice(begin, begin + rim)
            out_ref[0:rim] = x_one_ref[:, span, :]
            out_ref[rim : rim + size] = seed_ref[:, span, :]
            out_ref[rim + size :] = x_two_ref[:, span, :]

    @pl.when(even)
    def _():
        fill(one_ref, two_ref)

    @pl.when(jnp.logical_not(even))
    def _():
        fill(two_ref, one_ref)


def spread(wide_ref, rim, own, x_one, x_two, y_one, y_two):
    size, rows = own.shape
    shift = RIM - rim
    _, even_x = place_in(GX)
    _, even_y = place_in(GY)
    base_one = jnp.where(even_x, shift, RIM + size)
    base_two = shift + RIM + size - base_one


    def copy_own(k, carry):
        wide_ref[RIM + k, ROW : ROW + rows] = own.read(k)
        return carry

    lax.fori_loop(0, size, copy_own, 0)
    for k in range(rim):
        wide_ref[base_one + k, ROW : ROW + rows] = x_one(k)
        wide_ref[base_two + k, ROW : ROW + rows] = x_two(k)

    def edges(low, high):
        for k in range(size + 2 * rim):
            if k < rim:
                plane = base_one + k
            elif k < rim + size:
                plane = shift + k
            else:
                plane = base_two + k - rim - size
            wide_ref[plane, ROW - rim : ROW] = low(k)
            wide_ref[plane, ROW + rows : ROW + rows + rim] = high(k)

    @pl.when(even_y)
    def _():
        edges(y_one, y_two)

    @pl.when(jnp.logical_not(even_y))
    def _():
        edges(y_two, y_one)


class Own:
    def __init__(self, shape, read):
        self.shape = shape
        self.read = read


def pack_spot(at_x, at_y, at_z, depth):
    return ((at_x + RIM) * LINES + at_y + ROW) * depth + at_z


def unpack_spot(code, depth):
    line, at_z = split(code, depth)
    plane, row = split(line, LINES)
    return plane, row, at_z


def lay_kernel(
    grid_y,
    first_factor,
    second_factor,
    source_cells_ref,
    source_rate_ref,
    well_cells_ref,
    well_data_ref,
    well_weight_ref,
    cond_ref,
    root_ref,
    source_spot,
    first_amount,
    second_amount,
    well_spot,
    well_level,
    well_pull,
    source_cells,
    source_rate,
    well_cells,
    well_data,
    well_weight,
    done,
):
    copies = start_copies(
        (source_cells_ref, source_rate_ref, well_cells_ref, well_data_ref, well_weight_ref),
        (source_cells, source_rate, well_cells, well_data, well_weight),
        done,
    )
    size, rows, depth = cond_ref.shape
    place_x, _ = place_in(GX)
    place_y, _ = place_in(GY)
    anchor_x = place_x * size
    anchor_y = place_y * rows
    sources = source_cells.shape[0]
    wells = well_cells.shape[0]

    def own(k, carry):
        root_ref[k] = jnp.exp(0.5 * cond_ref[k])
        return carry

    lax.fori_loop(0, size, own, 0)
    for copy in copies:
        copy.wait()

    def spot(cell):
        line, at_z = split(cell, depth)
        at_x, at_y = split(line, grid_y)
        return at_x - anchor_x, at_y - anchor_y, at_z

    layer = grid_y * depth

    def outside(cell, rim):
        before = cell - (anchor_x - rim) * layer
        return before | ((size + 2 * rim) * layer - 1 - before)

    def check(cell, rim):
        _, at_y, _ = spot(cell)
        return (at_y >= -rim) & (at_y < rows + rim)

    source_spot[sources] = 0
    well_spot[wells] = 0

    def add_source(index):
        slot = source_spot[sources]
        source_spot[slot] = pack_spot(*spot(source_cells[index]), depth)
        first_amount[slot] = time_step * (source_rate[index] * first_factor[0])
        second_amount[slot] = time_step * (source_rate[index] * second_factor[0])
        source_spot[sources] = slot + 1

    visit(
        sources,
        lambda i: outside(source_cells[i], RIM - 1),
        lambda i: check(source_cells[i], RIM - 1),
        add_source,
    )

    def add_well(index):
        slot = well_spot[wells]
        well_spot[slot] = pack_spot(*spot(well_cells[index]), depth)
        well_level[slot] = well_data[index]
        well_pull[slot] = well_weight[index]
        well_spot[wells] = slot + 1

    visit(
        wells,
        lambda i: outside(well_cells[i], 0),
        lambda i: check(well_cells[i], 0),
        add_well,
    )


def sum_kernel(shares_ref, out_ref):
    total = jnp.sum(shares_ref[...], axis=0)
    for k in range(out_ref.shape[0]):
        out_ref[k] = total


def forward_kernel(
    grid_x,
    grid_y,
    source_spot_ref,
    first_amount_ref,
    second_amount_ref,
    well_spot_ref,
    well_level_ref,
    well_pull_ref,
    own_root_ref,
    start_ref,
    x_one_ref,
    x_two_ref,
    y_one_ref,
    y_two_ref,
    survey_ref,
    weight_ref,
    root_ref,
    state_ref,
    next_ref,
    final_ref,
    seed_ref,
    edge_one_ref,
    edge_two_ref,
    partial_ref,
    row_ref,
    flux_ref,
    source_spot,
    first_amount,
    second_amount,
    well_spot,
    well_level,
    well_pull,
    done,
):
    copies = start_copies(
        (
            source_spot_ref,
            first_amount_ref,
            second_amount_ref,
            well_spot_ref,
            well_level_ref,
            well_pull_ref,
        ),
        (source_spot, first_amount, second_amount, well_spot, well_level, well_pull),
        done,
    )
    size, rows, depth = survey_ref.shape
    wide = (root_ref.shape[1], depth)
    place_x, even_x = place_in(GX)
    place_y, _ = place_in(GY)
    anchor_x = place_x * size
    anchor_y = place_y * rows

    spread(
        state_ref,
        RIM,
        Own((size, rows), lambda k: start_ref[k]),
        lambda k: x_one_ref[0, k],
        lambda k: x_two_ref[0, k],
        lambda k: y_one_ref[0, k],
        lambda k: y_two_ref[0, k],
    )
    spread(
        root_ref,
        RIM,
        Own((size, rows), lambda k: own_root_ref[k]),
        lambda k: jnp.exp(0.5 * x_one_ref[1, k]),
        lambda k: jnp.exp(0.5 * x_two_ref[1, k]),
        lambda k: jnp.exp(0.5 * y_one_ref[1, k]),
        lambda k: jnp.exp(0.5 * y_two_ref[1, k]),
    )
    row_ref[...] = row_mask(wide, anchor_y, grid_y)
    open_z = lane_mask(wide)

    def along_x(ref, plane):
        here = ref[plane]
        ahead = ref[plane + 1]
        cond = root_ref[plane] * root_ref[plane + 1]
        flux = head_slope * cond * here - (molecular + dispersivity * cond) * (ahead - here)
        return flux * plane_mask(plane, anchor_x, grid_x)

    def advanced(ref, plane):
        here = ref[plane]
        root = root_ref[plane]
        flux_x = along_x(ref, plane)
        cond_y = root * up(root, 0)
        flux_y = (row_ref[...] * (molecular + dispersivity * cond_y)) * (here - up(here, 0))
        cond_z = root * up(root, 1)
        flux_z = (open_z * (molecular + dispersivity * cond_z)) * (here - up(here, 1))
        change = (flux_x - flux_ref[...]) + (flux_y - down(flux_y, 0)) + (flux_z - down(flux_z, 1))
        flux_ref[...] = flux_x
        return here - change

    lane = lax.broadcasted_iota(jnp.int32, (1, depth), 1)

    flux_ref[...] = along_x(state_ref, 0)

    def first_step(plane, carry):
        next_ref[plane] = advanced(state_ref, plane)
        return carry

    lax.fori_loop(1, size + 2 * RIM - 1, first_step, 0)

    for copy in copies:
        copy.wait()

    sources = source_spot[source_spot.shape[0] - PAD]

    def add_first(index, carry):
        plane, row, at_z = unpack_spot(source_spot[index], depth)
        where = (plane, pl.ds(row, 1), slice(None))
        next_ref[where] = next_ref[where] + jnp.where(lane == at_z, first_amount[index], 0.0)
        return carry

    lax.fori_loop(0, sources, add_first, 0)

    flux_ref[...] = along_x(next_ref, RIM - 1)

    def second_step(k, carry):
        final_ref[k] = advanced(next_ref, k + RIM)[ROW : ROW + rows]
        return carry

    lax.fori_loop(0, size, second_step, 0)

    def add_second(index, carry):
        plane, row, at_z = unpack_spot(source_spot[index], depth)
        plane = plane - RIM
        row = row - ROW

        @pl.when((plane >= 0) & (plane < size) & (row >= 0) & (row < rows))
        def _():
            where = (plane, pl.ds(row, 1), slice(None))
            amount = second_amount[index]
            final_ref[where] = final_ref[where] + jnp.where(lane == at_z, amount, 0.0)

        return carry

    lax.fori_loop(0, sources, add_second, 0)

    def compare(k, total):
        missed = final_ref[k] - survey_ref[k]
        seed = weight_ref[k] * missed
        seed_ref[k] = seed
        return total + jnp.sum((seed * missed).reshape(rows // 8, 8, depth), axis=0)

    total = lax.fori_loop(0, size, compare, jnp.zeros((8, depth), jnp.float32))

    def observe(index, total):
        plane, row, at_z = unpack_spot(well_spot[index], depth)
        where = (plane - RIM, pl.ds(row - ROW, 1), slice(None))
        nearby = final_ref[where] - well_level[index]
        pull = jnp.where(lane == at_z, well_pull[index] * nearby, 0.0)
        seed_ref[where] = seed_ref[where] + pull
        return total + pull * nearby

    wells = well_spot[well_spot.shape[0] - PAD]
    total = lax.fori_loop(0, wells, observe, jnp.sum(total, axis=0, keepdims=True))
    total = total * (0.5 / (grid_x * grid_y * depth))
    for k in range(partial_ref.shape[0]):
        partial_ref[k] = total

    first = jnp.where(even_x, 0, size - RIM)
    second = size - RIM - first
    for k in range(RIM):
        edge_one_ref[k] = seed_ref[first + k]
        edge_two_ref[k] = seed_ref[second + k]


def adjoint_kernel(
    grid_x,
    grid_y,
    root_ref,
    state_ref,
    next_ref,
    seed_ref,
    x_one_ref,
    x_two_ref,
    y_one_ref,
    y_two_ref,
    grad_ref,
    back_ref,
    last_ref,
    middle_ref,
    partial_ref,
    row_ref,
    pull_ref,
    sens_ref,
):
    size, rows, depth = seed_ref.shape
    wide = (root_ref.shape[1], depth)
    place_x, _ = place_in(GX)
    place_y, _ = place_in(GY)
    anchor_x = place_x * size
    anchor_y = place_y * rows
    spread(
        last_ref,
        RIM,
        Own((size, rows), lambda k: seed_ref[k]),
        lambda k: x_one_ref[k],
        lambda k: x_two_ref[k],
        lambda k: y_one_ref[k],
        lambda k: y_two_ref[k],
    )
    row_ref[...] = row_mask(wide, anchor_y, grid_y)
    open_z = lane_mask(wide)

    def along_x(adjoint_ref, tracer_ref, plane):
        jump = plane_mask(plane, anchor_x, grid_x) * (adjoint_ref[plane + 1] - adjoint_ref[plane])
        cond = root_ref[plane] * root_ref[plane + 1]
        pull = jump * (molecular + dispersivity * cond)
        push = jump * (head_slope * cond) + pull
        here = tracer_ref[plane]
        rise = head_slope * here - dispersivity * (tracer_ref[plane + 1] - here)
        return push, pull, jump * rise * (0.5 * cond)

    def along(adjoint, tracer, root, is_open, axis):
        jump = is_open * (up(adjoint, axis) - adjoint)
        cond = root * up(root, axis)
        pull = jump * (molecular + dispersivity * cond)
        sens = (jump * (tracer - up(tracer, axis))) * ((0.5 * dispersivity) * cond)
        return pull - down(pull, axis), sens + down(sens, axis)

    def reversed_step(adjoint_ref, tracer_ref, plane):
        push, pull, sens = along_x(adjoint_ref, tracer_ref, plane)
        adjoint = adjoint_ref[plane]
        tracer = tracer_ref[plane]
        root = root_ref[plane]
        change_y, sens_y = along(adjoint, tracer, root, row_ref[...], 0)
        change_z, sens_z = along(adjoint, tracer, root, open_z, 1)
        updated = adjoint + (push - pull_ref[...]) + change_y + change_z
        gradient = (sens + sens_ref[...]) + sens_y + sens_z
        pull_ref[...] = pull
        sens_ref[...] = sens
        return updated, gradient

    def begin(adjoint_ref, tracer_ref, plane):
        _, pull, sens = along_x(adjoint_ref, tracer_ref, plane)
        pull_ref[...] = pull
        sens_ref[...] = sens

    begin(last_ref, next_ref, RIM - 2)

    def later(plane, carry):
        updated, gradient = reversed_step(last_ref, next_ref, plane)
        middle_ref[plane] = updated
        partial_ref[plane] = gradient
        return carry

    lax.fori_loop(RIM - 1, size + RIM + 1, later, 0)

    begin(middle_ref, state_ref, RIM - 1)

    def earlier(k, carry):
        updated, gradient = reversed_step(middle_ref, state_ref, k + RIM)
        back_ref[k] = updated[ROW : ROW + rows]
        grad_ref[k] = (gradient + partial_ref[k + RIM])[ROW : ROW + rows]
        return carry

    lax.fori_loop(0, size, earlier, 0)


def call(kernel, outs, operands, *, scratch=(), flops=1_000_000, limit=2):
    shapes = tuple(
        space(shape, jnp.float32)
        if space == pltpu.VMEM
        else jax.ShapeDtypeStruct(*shape)
        if space == pltpu.SMEM
        else jax.ShapeDtypeStruct(shape, jnp.float32)
        for shape, space in outs
    )
    arrays = [
        array if space == pltpu.SMEM else pltpu.with_memory_space_constraint(array, space)
        for array, space in operands
    ]
    out_spaces = [pltpu.VMEM if space is None else space for _, space in outs]
    return pl.pallas_call(
        kernel,
        out_shape=shapes,
        in_specs=[pl.BlockSpec(memory_space=space) for _, space in operands],
        out_specs=tuple(pl.BlockSpec(memory_space=space) for space in out_spaces),
        scratch_shapes=scratch,
        cost_estimate=pl.CostEstimate(flops=flops, transcendentals=0, bytes_accessed=1_000_000),
        compiler_params=pltpu.CompilerParams(vmem_limit_bytes=limit << 20),
    )(*arrays)


def kept(*arrays, space=pltpu.VMEM):
    return tuple((array, space) for array in arrays)


def swapped(one, two, axes):
    count = lax.axis_size(axes)
    outer = [(i, i + 1) for i in range(1, count - 1, 2)]
    inner = [(i, i + 1) for i in range(0, count - 1, 2)]
    back = lambda pairs: pairs + [(b, a) for a, b in pairs]
    one = lax.ppermute(one, axes, back(outer))
    two = lax.ppermute(two, axes, back(inner))
    return one, two


def on_device(
    log_cond,
    checkpoint,
    survey,
    survey_weight,
    well_cells,
    well_data,
    well_weight,
    source_cells,
    source_rate,
    step_number,
):
    size, rows, depth = checkpoint.shape
    grid_x = size * lax.axis_size(GX)
    grid_y = rows * lax.axis_size(GY)
    clock = step_number.astype(jnp.float32)
    first_factor = 1.0 + 0.5 * jnp.sin(0.05 * clock)
    second_factor = 1.0 + 0.5 * jnp.sin(0.05 * (clock + 1.0))

    planes = size + 2 * RIM
    wide = (planes, rows + 2 * ROW, depth)
    flat = wide[1:]
    block = (size, rows, depth)
    f32 = functools.partial(pltpu.VMEM, dtype=jnp.float32)
    dma = pltpu.SemaphoreType.DMA

    x_edge = (2, RIM, rows, depth)
    x_one, x_two = call(
        pack_x_kernel,
        kept(x_edge, x_edge),
        kept(checkpoint, log_cond, space=pltpu.HBM),
        scratch=[dma((4,))],
    )
    x_one, x_two = swapped(x_one, x_two, GX)

    lists = (source_cells, source_rate, well_cells, well_data, well_weight)
    sources = source_cells.shape[0] + PAD
    wells = well_cells.shape[0] + PAD
    found = (
        ((sources,), jnp.int32),
        ((sources,), jnp.float32),
        ((sources,), jnp.float32),
        ((wells,), jnp.int32),
        ((wells,), jnp.float32),
        ((wells,), jnp.float32),
    )
    root, *hits = call(
        functools.partial(lay_kernel, grid_y),
        kept(block) + kept(*found, space=pltpu.SMEM),
        kept(first_factor, second_factor, space=pltpu.SMEM)
        + kept(*lists, space=pltpu.HBM)
        + kept(log_cond),
        scratch=[pltpu.SMEM(array.shape, array.dtype) for array in lists]
        + [dma((len(lists),))],
        flops=4_000_000,
    )

    y_edge = (2, planes, RIM, depth)
    y_one, y_two = call(
        pack_y_kernel, kept(y_edge, y_edge), kept(checkpoint, log_cond, x_one, x_two)
    )
    y_one, y_two = swapped(y_one, y_two, GY)

    s_edge = (RIM, rows, depth)
    near_axes = ("gx_1", GY)
    near_count = lax.axis_size(near_axes)
    fields = (root, checkpoint, x_one, x_two, y_one, y_two, survey, survey_weight)
    root, state, later, final, seed, s_one, s_two, partial = call(
        functools.partial(forward_kernel, grid_x, grid_y),
        kept(wide, wide, wide)
        + kept(block, space=None)
        + kept(block, s_edge, s_edge, (near_count, 1, depth)),
        kept(*hits) + kept(*fields),
        scratch=[f32(flat), f32(flat)]
        + [pltpu.SMEM(array.shape, array.dtype) for array in hits]
        + [dma((len(hits),))],
        flops=20_000_000,
        limit=4,
    )

    near = lax.all_to_all(partial, near_axes, 0, 0, tiled=True)
    (near,) = call(sum_kernel, kept((lax.axis_size(FAR), 1, depth)), kept(near))
    everyone = lax.all_to_all(near, FAR, 0, 0, tiled=True)
    misfit = jnp.sum(everyone).reshape(1)

    s_one, s_two = swapped(s_one, s_two, GX)
    t_edge = (planes, RIM, depth)
    t_one, t_two = call(pack_seed_kernel, kept(t_edge, t_edge), kept(seed, s_one, s_two))
    t_one, t_two = swapped(t_one, t_two, GY)
    grad, back = call(
        functools.partial(adjoint_kernel, grid_x, grid_y),
        kept(block, block, space=None),
        kept(root, state, later, seed, s_one, s_two, t_one, t_two),
        scratch=[f32(wide)] * 3 + [f32(flat)] * 3,
        flops=20_000_000,
        limit=6,
    )
    return (grad, back, final, misfit)


def solution(mesh):
    ens, along_x, along_y = (mesh.shape[name] for name in ("ens", "gx", "gy"))
    finer = Mesh(
        mesh.devices.reshape(ens, along_x // 2, 2, along_y), ("ens", "gx_0", "gx_1", "gy")
    )
    field = P(ENS_GX, "gy", None)

    return jax.shard_map(
        on_device,
        mesh=finer,
        in_specs=(field,) * 4 + (P("ens"),) * 6,
        out_specs=(field, field, field, P("ens")),
        check_vma=False,
    )
```

```python
import functools
import math
import operator

import jax
import jax.numpy as jnp
from jax import lax
from jax.experimental import pallas as pl
from jax.experimental.pallas import tpu as pltpu
from jax.sharding import Mesh
from jax.sharding import PartitionSpec as P

FAR = "gx_0"
GX = ("gx_0", "gx_1")
GY = "gy"
ENS_GX = ("ens", "gx_0", "gx_1")

time_step = 0.2
head_slope = 0.5
molecular = 0.05
dispersivity = 0.1

RIM = 2
ROW = 8
LINES = 1024
PAD = 8


def split(value, size):
    if size & (size - 1) == 0:
        return value >> (size.bit_length() - 1), value & (size - 1)
    return lax.div(value, jnp.int32(size)), lax.rem(value, jnp.int32(size))


def place_in(axes):
    position = lax.axis_index(axes)
    return position, position % 2 == 0


def up(field, axis):
    return pltpu.roll(field, field.shape[axis] - 1, axis)


def down(field, axis):
    return pltpu.roll(field, 1, axis)


def lane_mask(shape):
    lane = lax.broadcasted_iota(jnp.int32, shape, 1)
    return jnp.where(lane < shape[1] - 1, jnp.float32(time_step), jnp.float32(0.0))


def row_mask(shape, first, total):
    position = lax.broadcasted_iota(jnp.int32, shape, 0) - ROW + first
    is_open = (position >= 0) & (position + 1 < total)
    return jnp.where(is_open, jnp.float32(time_step), jnp.float32(0.0))


def plane_mask(plane, first, total):
    position = first - RIM + plane
    is_open = (position >= 0) & (position + 1 < total)
    return jnp.where(is_open, jnp.float32(time_step), jnp.float32(0.0))


def visit(count, far, outside, act):
    group = math.gcd(count, 8)

    def none_of(test, base):
        return functools.reduce(operator.and_, [test(base + k) for k in range(group)])

    def one(index):
        @pl.when(outside(index) >= 0)
        def _():
            act(index)

    def step(number, carry):
        base = number * group

        @pl.when(none_of(far, base) >= 0)
        def _():
            @pl.when(none_of(outside, base) >= 0)
            def _():
                lax.fori_loop(0, group, lambda k, c: (one(base + k), c)[1], 0)

        return carry

    lax.fori_loop(0, count // group, step, 0)


def start_copies(sources, targets, done):
    copies = [
        pltpu.make_async_copy(source, target, done.at[k])
        for k, (source, target) in enumerate(zip(sources, targets))
    ]
    for copy in copies:
        copy.start()
    return copies


def pack_x_kernel(start_ref, cond_ref, one_ref, two_ref, done):
    size = start_ref.shape[0]
    _, even = place_in(GX)
    first = jnp.where(even, 0, size - RIM)
    second = size - RIM - first
    copies = []
    for out_ref, begin in ((one_ref, first), (two_ref, second)):
        for which, own_ref in ((0, start_ref), (1, cond_ref)):
            source = own_ref.at[pl.ds(begin, RIM)]
            copies.append(
                pltpu.make_async_copy(source, out_ref.at[which], done.at[len(copies)])
            )
    for copy in copies:
        copy.start()
    for copy in copies:
        copy.wait()


def pack_y_kernel(start_ref, cond_ref, x_one_ref, x_two_ref, out_ref):
    size, rows = start_ref.shape[:2]
    place = lax.axis_index(GY)
    out_ref[place] = jnp.zeros(out_ref.shape[1:], jnp.float32)

    def fill(slot, begin):
        span = slice(begin, begin + RIM)
        for which, own_ref in ((0, start_ref), (1, cond_ref)):
            out_ref[slot, which, 0:RIM] = x_one_ref[which, :, span, :]
            out_ref[slot, which, RIM : RIM + size] = own_ref[:, span, :]
            out_ref[slot, which, RIM + size :] = x_two_ref[which, :, span, :]

    @pl.when(place > 0)
    def _():
        fill(place - 1, 0)

    @pl.when(place < out_ref.shape[0] - 1)
    def _():
        fill(place + 1, rows - RIM)


def pack_seed_kernel(seed_ref, x_one_ref, x_two_ref, one_ref, two_ref):
    size, rows = seed_ref.shape[:2]
    rim = RIM
    _, even = place_in(GY)

    def fill(low_ref, high_ref):
        for out_ref, begin in ((low_ref, 0), (high_ref, rows - rim)):
            span = slice(begin, begin + rim)
            out_ref[0:rim] = x_one_ref[:, span, :]
            out_ref[rim : rim + size] = seed_ref[:, span, :]
            out_ref[rim + size :] = x_two_ref[:, span, :]

    @pl.when(even)
    def _():
        fill(one_ref, two_ref)

    @pl.when(jnp.logical_not(even))
    def _():
        fill(two_ref, one_ref)


def spread(wide_ref, rim, own, x_one, x_two, y_one, y_two, y_sorted=False):
    size, rows = own.shape
    shift = RIM - rim
    _, even_x = place_in(GX)
    _, even_y = place_in(GY)
    base_one = jnp.where(even_x, shift, RIM + size)
    base_two = shift + RIM + size - base_one


    def copy_own(k, carry):
        wide_ref[RIM + k, ROW : ROW + rows] = own.read(k)
        return carry

    lax.fori_loop(0, size, copy_own, 0)
    for k in range(rim):
        wide_ref[base_one + k, ROW : ROW + rows] = x_one(k)
        wide_ref[base_two + k, ROW : ROW + rows] = x_two(k)

    def edges(low, high):
        for k in range(size + 2 * rim):
            if k < rim:
                plane = base_one + k
            elif k < rim + size:
                plane = shift + k
            else:
                plane = base_two + k - rim - size
            wide_ref[plane, ROW - rim : ROW] = low(k)
            wide_ref[plane, ROW + rows : ROW + rows + rim] = high(k)

    if y_sorted:
        edges(y_one, y_two)
        return

    @pl.when(even_y)
    def _():
        edges(y_one, y_two)

    @pl.when(jnp.logical_not(even_y))
    def _():
        edges(y_two, y_one)


class Own:
    def __init__(self, shape, read):
        self.shape = shape
        self.read = read


def pack_spot(at_x, at_y, at_z, depth):
    return ((at_x + RIM) * LINES + at_y + ROW) * depth + at_z


def unpack_spot(code, depth):
    line, at_z = split(code, depth)
    plane, row = split(line, LINES)
    return plane, row, at_z


def lay_kernel(
    grid_y,
    first_factor,
    second_factor,
    source_cells_ref,
    source_rate_ref,
    well_cells_ref,
    well_data_ref,
    well_weight_ref,
    cond_ref,
    root_ref,
    source_spot,
    first_amount,
    second_amount,
    well_spot,
    well_level,
    well_pull,
    source_cells,
    source_rate,
    well_cells,
    well_data,
    well_weight,
    done,
):
    copies = start_copies(
        (source_cells_ref, source_rate_ref, well_cells_ref, well_data_ref, well_weight_ref),
        (source_cells, source_rate, well_cells, well_data, well_weight),
        done,
    )
    size, rows, depth = cond_ref.shape
    place_x, _ = place_in(GX)
    place_y, _ = place_in(GY)
    anchor_x = place_x * size
    anchor_y = place_y * rows
    sources = source_cells.shape[0]
    wells = well_cells.shape[0]

    def own(k, carry):
        root_ref[k] = jnp.exp(0.5 * cond_ref[k])
        return carry

    lax.fori_loop(0, size, own, 0)
    for copy in copies:
        copy.wait()

    def spot(cell):
        line, at_z = split(cell, depth)
        at_x, at_y = split(line, grid_y)
        return at_x - anchor_x, at_y - anchor_y, at_z

    layer = grid_y * depth

    layer = grid_y * depth

    def far(cell, rim):
        before = cell - (anchor_x - rim) * layer
        return before | ((size + 2 * rim) * layer - 1 - before)

    def outside(cell, rim):
        at_x, at_y, _ = spot(cell)
        return (
            (at_x + rim) | (size - 1 + rim - at_x) | (at_y + rim) | (rows - 1 + rim - at_y)
        )

    source_spot[sources] = 0
    well_spot[wells] = 0

    def add_source(index):
        slot = source_spot[sources]
        source_spot[slot] = pack_spot(*spot(source_cells[index]), depth)
        first_amount[slot] = time_step * (source_rate[index] * first_factor[0])
        second_amount[slot] = time_step * (source_rate[index] * second_factor[0])
        source_spot[sources] = slot + 1

    visit(
        sources,
        lambda i: far(source_cells[i], RIM - 1),
        lambda i: outside(source_cells[i], RIM - 1),
        add_source,
    )

    def add_well(index):
        slot = well_spot[wells]
        well_spot[slot] = pack_spot(*spot(well_cells[index]), depth)
        well_level[slot] = well_data[index]
        well_pull[slot] = well_weight[index]
        well_spot[wells] = slot + 1

    visit(
        wells,
        lambda i: far(well_cells[i], 0),
        lambda i: outside(well_cells[i], 0),
        add_well,
    )


def sum_kernel(shares_ref, out_ref):
    total = jnp.sum(shares_ref[...], axis=0)
    for k in range(out_ref.shape[0]):
        out_ref[k] = total


def forward_kernel(
    grid_x,
    grid_y,
    source_spot_ref,
    first_amount_ref,
    second_amount_ref,
    well_spot_ref,
    well_level_ref,
    well_pull_ref,
    own_root_ref,
    start_ref,
    x_one_ref,
    x_two_ref,
    y_ref,
    survey_ref,
    weight_ref,
    root_ref,
    state_ref,
    next_ref,
    final_ref,
    seed_ref,
    edge_one_ref,
    edge_two_ref,
    partial_ref,
    row_ref,
    flux_ref,
    source_spot,
    first_amount,
    second_amount,
    well_spot,
    well_level,
    well_pull,
    done,
):
    copies = start_copies(
        (
            source_spot_ref,
            first_amount_ref,
            second_amount_ref,
            well_spot_ref,
            well_level_ref,
            well_pull_ref,
        ),
        (source_spot, first_amount, second_amount, well_spot, well_level, well_pull),
        done,
    )
    size, rows, depth = survey_ref.shape
    wide = (root_ref.shape[1], depth)
    place_x, even_x = place_in(GX)
    place_y = lax.axis_index(GY)
    anchor_x = place_x * size
    anchor_y = place_y * rows
    low = jnp.maximum(place_y - 1, 0)
    high = jnp.minimum(place_y + 1, y_ref.shape[0] - 1)

    spread(
        state_ref,
        RIM,
        Own((size, rows), lambda k: start_ref[k]),
        lambda k: x_one_ref[0, k],
        lambda k: x_two_ref[0, k],
        lambda k: y_ref[low, 0, k],
        lambda k: y_ref[high, 0, k],
        y_sorted=True,
    )
    spread(
        root_ref,
        RIM,
        Own((size, rows), lambda k: own_root_ref[k]),
        lambda k: jnp.exp(0.5 * x_one_ref[1, k]),
        lambda k: jnp.exp(0.5 * x_two_ref[1, k]),
        lambda k: jnp.exp(0.5 * y_ref[low, 1, k]),
        lambda k: jnp.exp(0.5 * y_ref[high, 1, k]),
        y_sorted=True,
    )
    row_ref[...] = row_mask(wide, anchor_y, grid_y)
    open_z = lane_mask(wide)

    def along_x(ref, plane):
        here = ref[plane]
        ahead = ref[plane + 1]
        cond = root_ref[plane] * root_ref[plane + 1]
        flux = head_slope * cond * here - (molecular + dispersivity * cond) * (ahead - here)
        return flux * plane_mask(plane, anchor_x, grid_x)

    def advanced(ref, plane):
        here = ref[plane]
        root = root_ref[plane]
        flux_x = along_x(ref, plane)
        cond_y = root * up(root, 0)
        flux_y = (row_ref[...] * (molecular + dispersivity * cond_y)) * (here - up(here, 0))
        cond_z = root * up(root, 1)
        flux_z = (open_z * (molecular + dispersivity * cond_z)) * (here - up(here, 1))
        change = (flux_x - flux_ref[...]) + (flux_y - down(flux_y, 0)) + (flux_z - down(flux_z, 1))
        flux_ref[...] = flux_x
        return here - change

    lane = lax.broadcasted_iota(jnp.int32, (1, depth), 1)

    flux_ref[...] = along_x(state_ref, 0)

    def first_step(plane, carry):
        next_ref[plane] = advanced(state_ref, plane)
        return carry

    lax.fori_loop(1, size + 2 * RIM - 1, first_step, 0)

    for copy in copies:
        copy.wait()

    sources = source_spot[source_spot.shape[0] - PAD]

    def add_first(index, carry):
        plane, row, at_z = unpack_spot(source_spot[index], depth)
        where = (plane, pl.ds(row, 1), slice(None))
        next_ref[where] = next_ref[where] + jnp.where(lane == at_z, first_amount[index], 0.0)
        return carry

    lax.fori_loop(0, sources, add_first, 0)

    flux_ref[...] = along_x(next_ref, RIM - 1)

    def second_step(k, carry):
        final_ref[k] = advanced(next_ref, k + RIM)[ROW : ROW + rows]
        return carry

    lax.fori_loop(0, size, second_step, 0)

    def add_second(index, carry):
        plane, row, at_z = unpack_spot(source_spot[index], depth)
        plane = plane - RIM
        row = row - ROW

        @pl.when((plane >= 0) & (plane < size) & (row >= 0) & (row < rows))
        def _():
            where = (plane, pl.ds(row, 1), slice(None))
            amount = second_amount[index]
            final_ref[where] = final_ref[where] + jnp.where(lane == at_z, amount, 0.0)

        return carry

    lax.fori_loop(0, sources, add_second, 0)

    def compare(k, total):
        missed = final_ref[k] - survey_ref[k]
        seed = weight_ref[k] * missed
        seed_ref[k] = seed
        return total + jnp.sum((seed * missed).reshape(rows // 8, 8, depth), axis=0)

    total = lax.fori_loop(0, size, compare, jnp.zeros((8, depth), jnp.float32))

    def observe(index, total):
        plane, row, at_z = unpack_spot(well_spot[index], depth)
        where = (plane - RIM, pl.ds(row - ROW, 1), slice(None))
        nearby = final_ref[where] - well_level[index]
        pull = jnp.where(lane == at_z, well_pull[index] * nearby, 0.0)
        seed_ref[where] = seed_ref[where] + pull
        return total + pull * nearby

    wells = well_spot[well_spot.shape[0] - PAD]
    total = lax.fori_loop(0, wells, observe, jnp.sum(total, axis=0, keepdims=True))
    total = total * (0.5 / (grid_x * grid_y * depth))
    for k in range(partial_ref.shape[0]):
        partial_ref[k] = total

    first = jnp.where(even_x, 0, size - RIM)
    second = size - RIM - first
    for k in range(RIM):
        edge_one_ref[k] = seed_ref[first + k]
        edge_two_ref[k] = seed_ref[second + k]


def adjoint_kernel(
    grid_x,
    grid_y,
    root_ref,
    state_ref,
    next_ref,
    seed_ref,
    x_one_ref,
    x_two_ref,
    y_one_ref,
    y_two_ref,
    grad_ref,
    back_ref,
    last_ref,
    middle_ref,
    partial_ref,
    row_ref,
    pull_ref,
    sens_ref,
):
    size, rows, depth = seed_ref.shape
    wide = (root_ref.shape[1], depth)
    place_x, _ = place_in(GX)
    place_y, _ = place_in(GY)
    anchor_x = place_x * size
    anchor_y = place_y * rows
    spread(
        last_ref,
        RIM,
        Own((size, rows), lambda k: seed_ref[k]),
        lambda k: x_one_ref[k],
        lambda k: x_two_ref[k],
        lambda k: y_one_ref[k],
        lambda k: y_two_ref[k],
    )
    row_ref[...] = row_mask(wide, anchor_y, grid_y)
    open_z = lane_mask(wide)

    def along_x(adjoint_ref, tracer_ref, plane):
        jump = plane_mask(plane, anchor_x, grid_x) * (adjoint_ref[plane + 1] - adjoint_ref[plane])
        cond = root_ref[plane] * root_ref[plane + 1]
        pull = jump * (molecular + dispersivity * cond)
        push = jump * (head_slope * cond) + pull
        here = tracer_ref[plane]
        rise = head_slope * here - dispersivity * (tracer_ref[plane + 1] - here)
        return push, pull, jump * rise * (0.5 * cond)

    def along(adjoint, tracer, root, is_open, axis):
        jump = is_open * (up(adjoint, axis) - adjoint)
        cond = root * up(root, axis)
        pull = jump * (molecular + dispersivity * cond)
        sens = (jump * (tracer - up(tracer, axis))) * ((0.5 * dispersivity) * cond)
        return pull - down(pull, axis), sens + down(sens, axis)

    def reversed_step(adjoint_ref, tracer_ref, plane):
        push, pull, sens = along_x(adjoint_ref, tracer_ref, plane)
        adjoint = adjoint_ref[plane]
        tracer = tracer_ref[plane]
        root = root_ref[plane]
        change_y, sens_y = along(adjoint, tracer, root, row_ref[...], 0)
        change_z, sens_z = along(adjoint, tracer, root, open_z, 1)
        updated = adjoint + (push - pull_ref[...]) + change_y + change_z
        gradient = (sens + sens_ref[...]) + sens_y + sens_z
        pull_ref[...] = pull
        sens_ref[...] = sens
        return updated, gradient

    def begin(adjoint_ref, tracer_ref, plane):
        _, pull, sens = along_x(adjoint_ref, tracer_ref, plane)
        pull_ref[...] = pull
        sens_ref[...] = sens

    begin(last_ref, next_ref, RIM - 2)

    def later(plane, carry):
        updated, gradient = reversed_step(last_ref, next_ref, plane)
        middle_ref[plane] = updated
        partial_ref[plane] = gradient
        return carry

    lax.fori_loop(RIM - 1, size + RIM + 1, later, 0)

    begin(middle_ref, state_ref, RIM - 1)

    def earlier(k, carry):
        updated, gradient = reversed_step(middle_ref, state_ref, k + RIM)
        back_ref[k] = updated[ROW : ROW + rows]
        grad_ref[k] = (gradient + partial_ref[k + RIM])[ROW : ROW + rows]
        return carry

    lax.fori_loop(0, size, earlier, 0)


def call(kernel, outs, operands, *, scratch=(), flops=1_000_000, limit=2):
    shapes = tuple(
        space(shape, jnp.float32)
        if space == pltpu.VMEM
        else jax.ShapeDtypeStruct(*shape)
        if space == pltpu.SMEM
        else jax.ShapeDtypeStruct(shape, jnp.float32)
        for shape, space in outs
    )
    arrays = [
        array if space == pltpu.SMEM else pltpu.with_memory_space_constraint(array, space)
        for array, space in operands
    ]
    out_spaces = [pltpu.VMEM if space is None else space for _, space in outs]
    return pl.pallas_call(
        kernel,
        out_shape=shapes,
        in_specs=[pl.BlockSpec(memory_space=space) for _, space in operands],
        out_specs=tuple(pl.BlockSpec(memory_space=space) for space in out_spaces),
        scratch_shapes=scratch,
        cost_estimate=pl.CostEstimate(flops=flops, transcendentals=0, bytes_accessed=1_000_000),
        compiler_params=pltpu.CompilerParams(vmem_limit_bytes=limit << 20),
    )(*arrays)


def kept(*arrays, space=pltpu.VMEM):
    return tuple((array, space) for array in arrays)


def swapped(one, two, axes):
    count = lax.axis_size(axes)
    outer = [(i, i + 1) for i in range(1, count - 1, 2)]
    inner = [(i, i + 1) for i in range(0, count - 1, 2)]
    back = lambda pairs: pairs + [(b, a) for a, b in pairs]
    one = lax.ppermute(one, axes, back(outer))
    two = lax.ppermute(two, axes, back(inner))
    return one, two


def on_device(
    log_cond,
    checkpoint,
    survey,
    survey_weight,
    well_cells,
    well_data,
    well_weight,
    source_cells,
    source_rate,
    step_number,
):
    size, rows, depth = checkpoint.shape
    grid_x = size * lax.axis_size(GX)
    grid_y = rows * lax.axis_size(GY)
    clock = step_number.astype(jnp.float32)
    first_factor = 1.0 + 0.5 * jnp.sin(0.05 * clock)
    second_factor = 1.0 + 0.5 * jnp.sin(0.05 * (clock + 1.0))

    planes = size + 2 * RIM
    wide = (planes, rows + 2 * ROW, depth)
    flat = wide[1:]
    block = (size, rows, depth)
    f32 = functools.partial(pltpu.VMEM, dtype=jnp.float32)
    dma = pltpu.SemaphoreType.DMA

    x_edge = (2, RIM, rows, depth)
    x_one, x_two = call(
        pack_x_kernel,
        kept(x_edge, x_edge),
        kept(checkpoint, log_cond, space=pltpu.HBM),
        scratch=[dma((4,))],
    )
    x_one, x_two = swapped(x_one, x_two, GX)

    lists = (source_cells, source_rate, well_cells, well_data, well_weight)
    sources = source_cells.shape[0] + PAD
    wells = well_cells.shape[0] + PAD
    found = (
        ((sources,), jnp.int32),
        ((sources,), jnp.float32),
        ((sources,), jnp.float32),
        ((wells,), jnp.int32),
        ((wells,), jnp.float32),
        ((wells,), jnp.float32),
    )
    root, *hits = call(
        functools.partial(lay_kernel, grid_y),
        kept(block) + kept(*found, space=pltpu.SMEM),
        kept(first_factor, second_factor, space=pltpu.SMEM)
        + kept(*lists, space=pltpu.HBM)
        + kept(log_cond),
        scratch=[pltpu.SMEM(array.shape, array.dtype) for array in lists]
        + [dma((len(lists),))],
        flops=4_000_000,
    )

    y_slots = (lax.axis_size(GY), 2, planes, RIM, depth)
    (edges,) = call(pack_y_kernel, kept(y_slots), kept(checkpoint, log_cond, x_one, x_two))
    edges = lax.all_to_all(edges, GY, 0, 0, tiled=True)

    s_edge = (RIM, rows, depth)
    near_axes = ("gx_1", GY)
    near_count = lax.axis_size(near_axes)
    fields = (root, checkpoint, x_one, x_two, edges, survey, survey_weight)
    root, state, later, final, seed, s_one, s_two, partial = call(
        functools.partial(forward_kernel, grid_x, grid_y),
        kept(wide, wide, wide)
        + kept(block, space=None)
        + kept(block, s_edge, s_edge, (near_count, 1, depth)),
        kept(*hits) + kept(*fields),
        scratch=[f32(flat), f32(flat)]
        + [pltpu.SMEM(array.shape, array.dtype) for array in hits]
        + [dma((len(hits),))],
        flops=20_000_000,
        limit=4,
    )

    near = lax.all_to_all(partial, near_axes, 0, 0, tiled=True)
    (near,) = call(sum_kernel, kept((lax.axis_size(FAR), 1, depth)), kept(near))
    everyone = lax.all_to_all(near, FAR, 0, 0, tiled=True)
    misfit = jnp.sum(everyone).reshape(1)

    s_one, s_two = swapped(s_one, s_two, GX)
    t_edge = (planes, RIM, depth)
    t_one, t_two = call(pack_seed_kernel, kept(t_edge, t_edge), kept(seed, s_one, s_two))
    t_one, t_two = swapped(t_one, t_two, GY)
    grad, back = call(
        functools.partial(adjoint_kernel, grid_x, grid_y),
        kept(block, block, space=None),
        kept(root, state, later, seed, s_one, s_two, t_one, t_two),
        scratch=[f32(wide)] * 3 + [f32(flat)] * 3,
        flops=20_000_000,
        limit=6,
    )
    return (grad, back, final, misfit)


def solution(mesh):
    ens, along_x, along_y = (mesh.shape[name] for name in ("ens", "gx", "gy"))
    finer = Mesh(
        mesh.devices.reshape(ens, along_x // 2, 2, along_y), ("ens", "gx_0", "gx_1", "gy")
    )
    field = P(ENS_GX, "gy", None)

    return jax.shard_map(
        on_device,
        mesh=finer,
        in_specs=(field,) * 4 + (P("ens"),) * 6,
        out_specs=(field, field, field, P("ens")),
        check_vma=False,
    )
```

```python
import functools
import math
import operator

import jax
import jax.numpy as jnp
from jax import lax
from jax.experimental import pallas as pl
from jax.experimental.pallas import tpu as pltpu
from jax.sharding import Mesh
from jax.sharding import PartitionSpec as P

FAR = "gx_0"
GX = ("gx_0", "gx_1")
GY = "gy"
ENS_GX = ("ens", "gx_0", "gx_1")

time_step = 0.2
head_slope = 0.5
molecular = 0.05
dispersivity = 0.1

RIM = 2
ROW = 8
LINES = 1024
PAD = 8


def split(value, size):
    if size & (size - 1) == 0:
        return value >> (size.bit_length() - 1), value & (size - 1)
    return lax.div(value, jnp.int32(size)), lax.rem(value, jnp.int32(size))


def place_in(axes):
    position = lax.axis_index(axes)
    return position, position % 2 == 0


def up(field, axis):
    return pltpu.roll(field, field.shape[axis] - 1, axis)


def down(field, axis):
    return pltpu.roll(field, 1, axis)


def lane_mask(shape):
    lane = lax.broadcasted_iota(jnp.int32, shape, 1)
    return jnp.where(lane < shape[1] - 1, jnp.float32(time_step), jnp.float32(0.0))


def row_mask(shape, first, total):
    position = lax.broadcasted_iota(jnp.int32, shape, 0) - ROW + first
    is_open = (position >= 0) & (position + 1 < total)
    return jnp.where(is_open, jnp.float32(time_step), jnp.float32(0.0))


def plane_mask(plane, first, total):
    position = first - RIM + plane
    is_open = (position >= 0) & (position + 1 < total)
    return jnp.where(is_open, jnp.float32(time_step), jnp.float32(0.0))


def visit(count, far, outside, act):
    group = math.gcd(count, 8)

    def none_of(test, base):
        return functools.reduce(operator.and_, [test(base + k) for k in range(group)])

    def one(index):
        @pl.when(outside(index) >= 0)
        def _():
            act(index)

    def step(number, carry):
        base = number * group

        @pl.when(none_of(far, base) >= 0)
        def _():
            @pl.when(none_of(outside, base) >= 0)
            def _():
                lax.fori_loop(0, group, lambda k, c: (one(base + k), c)[1], 0)

        return carry

    lax.fori_loop(0, count // group, step, 0)


def start_copies(sources, targets, done):
    copies = [
        pltpu.make_async_copy(source, target, done.at[k])
        for k, (source, target) in enumerate(zip(sources, targets))
    ]
    for copy in copies:
        copy.start()
    return copies


def pack_x_kernel(start_ref, cond_ref, one_ref, two_ref, done):
    size = start_ref.shape[0]
    _, even = place_in(GX)
    first = jnp.where(even, 0, size - RIM)
    second = size - RIM - first
    copies = []
    for out_ref, begin in ((one_ref, first), (two_ref, second)):
        for which, own_ref in ((0, start_ref), (1, cond_ref)):
            source = own_ref.at[pl.ds(begin, RIM)]
            copies.append(
                pltpu.make_async_copy(source, out_ref.at[which], done.at[len(copies)])
            )
    for copy in copies:
        copy.start()
    for copy in copies:
        copy.wait()


def pack_y_kernel(start_ref, cond_ref, x_one_ref, x_two_ref, one_ref, two_ref):
    size, rows = start_ref.shape[:2]
    _, even = place_in(GY)

    def fill(low_ref, high_ref):
        for out_ref, begin in ((low_ref, 0), (high_ref, rows - RIM)):
            span = slice(begin, begin + RIM)
            for which, own_ref in ((0, start_ref), (1, cond_ref)):
                out_ref[which, 0:RIM] = x_one_ref[which, :, span, :]
                out_ref[which, RIM : RIM + size] = own_ref[:, span, :]
                out_ref[which, RIM + size :] = x_two_ref[which, :, span, :]

    @pl.when(even)
    def _():
        fill(one_ref, two_ref)

    @pl.when(jnp.logical_not(even))
    def _():
        fill(two_ref, one_ref)


def pack_seed_kernel(seed_ref, x_one_ref, x_two_ref, one_ref, two_ref):
    size, rows = seed_ref.shape[:2]
    rim = RIM
    _, even = place_in(GY)

    def fill(low_ref, high_ref):
        for out_ref, begin in ((low_ref, 0), (high_ref, rows - rim)):
            span = slice(begin, begin + rim)
            out_ref[0:rim] = x_one_ref[:, span, :]
            out_ref[rim : rim + size] = seed_ref[:, span, :]
            out_ref[rim + size :] = x_two_ref[:, span, :]

    @pl.when(even)
    def _():
        fill(one_ref, two_ref)

    @pl.when(jnp.logical_not(even))
    def _():
        fill(two_ref, one_ref)


def spread(wide_ref, rim, own, x_one, x_two, y_one, y_two):
    size, rows = own.shape
    shift = RIM - rim
    _, even_x = place_in(GX)
    _, even_y = place_in(GY)
    base_one = jnp.where(even_x, shift, RIM + size)
    base_two = shift + RIM + size - base_one


    def copy_own(k, carry):
        wide_ref[RIM + k, ROW : ROW + rows] = own.read(k)
        return carry

    lax.fori_loop(0, size, copy_own, 0)
    for k in range(rim):
        wide_ref[base_one + k, ROW : ROW + rows] = x_one(k)
        wide_ref[base_two + k, ROW : ROW + rows] = x_two(k)

    def edges(low, high):
        for k in range(size + 2 * rim):
            if k < rim:
                plane = base_one + k
            elif k < rim + size:
                plane = shift + k
            else:
                plane = base_two + k - rim - size
            wide_ref[plane, ROW - rim : ROW] = low(k)
            wide_ref[plane, ROW + rows : ROW + rows + rim] = high(k)

    @pl.when(even_y)
    def _():
        edges(y_one, y_two)

    @pl.when(jnp.logical_not(even_y))
    def _():
        edges(y_two, y_one)


class Own:
    def __init__(self, shape, read):
        self.shape = shape
        self.read = read


def pack_spot(at_x, at_y, at_z, depth):
    return ((at_x + RIM) * LINES + at_y + ROW) * depth + at_z


def unpack_spot(code, depth):
    line, at_z = split(code, depth)
    plane, row = split(line, LINES)
    return plane, row, at_z


def finder(size, rows, depth, grid_y):
    anchor_x = lax.axis_index(GX) * size
    anchor_y = lax.axis_index(GY) * rows
    layer = grid_y * depth

    def spot(cell):
        line, at_z = split(cell, depth)
        at_x, at_y = split(line, grid_y)
        return at_x - anchor_x, at_y - anchor_y, at_z

    def far(cell, rim):
        before = cell - (anchor_x - rim) * layer
        return before | ((size + 2 * rim) * layer - 1 - before)

    def outside(cell, rim):
        at_x, at_y, _ = spot(cell)
        return (
            (at_x + rim) | (size - 1 + rim - at_x) | (at_y + rim) | (rows - 1 + rim - at_y)
        )

    def packed(cell):
        return pack_spot(*spot(cell), depth)

    return far, outside, packed


def lay_kernel(
    grid_y,
    first_factor,
    second_factor,
    cells_ref,
    rate_ref,
    cond_ref,
    root_ref,
    spot_ref,
    first_ref,
    second_ref,
    cells,
    rate,
    done,
):
    copies = start_copies((cells_ref, rate_ref), (cells, rate), done)
    size, rows, depth = cond_ref.shape
    count = cells.shape[0]

    def own(k, carry):
        root_ref[k] = jnp.exp(0.5 * cond_ref[k])
        return carry

    lax.fori_loop(0, size, own, 0)
    for copy in copies:
        copy.wait()
    far, outside, packed = finder(size, rows, depth, grid_y)
    spot_ref[count] = 0

    def add(index):
        slot = spot_ref[count]
        spot_ref[slot] = packed(cells[index])
        first_ref[slot] = time_step * (rate[index] * first_factor[0])
        second_ref[slot] = time_step * (rate[index] * second_factor[0])
        spot_ref[count] = slot + 1

    visit(
        count,
        lambda i: far(cells[i], RIM - 1),
        lambda i: outside(cells[i], RIM - 1),
        add,
    )


def find_kernel(
    block,
    grid_y,
    cells_ref,
    data_ref,
    weight_ref,
    spot_ref,
    level_ref,
    pull_ref,
    cells,
    data,
    weight,
    done,
):
    copies = start_copies((cells_ref, data_ref, weight_ref), (cells, data, weight), done)
    count = cells.shape[0]
    far, outside, packed = finder(*block, grid_y)
    spot_ref[count] = 0
    for copy in copies:
        copy.wait()

    def add(index):
        slot = spot_ref[count]
        spot_ref[slot] = packed(cells[index])
        level_ref[slot] = data[index]
        pull_ref[slot] = weight[index]
        spot_ref[count] = slot + 1

    visit(count, lambda i: far(cells[i], 0), lambda i: outside(cells[i], 0), add)


def sum_kernel(shares_ref, out_ref):
    total = jnp.sum(shares_ref[...], axis=0)
    for k in range(out_ref.shape[0]):
        out_ref[k] = total


def forward_kernel(
    grid_x,
    grid_y,
    source_spot_ref,
    first_amount_ref,
    second_amount_ref,
    well_spot_ref,
    well_level_ref,
    well_pull_ref,
    own_root_ref,
    start_ref,
    x_one_ref,
    x_two_ref,
    y_one_ref,
    y_two_ref,
    survey_ref,
    weight_ref,
    root_ref,
    state_ref,
    next_ref,
    final_ref,
    seed_ref,
    edge_one_ref,
    edge_two_ref,
    partial_ref,
    row_ref,
    flux_ref,
    source_spot,
    first_amount,
    second_amount,
    well_spot,
    well_level,
    well_pull,
    done,
):
    copies = start_copies(
        (
            source_spot_ref,
            first_amount_ref,
            second_amount_ref,
            well_spot_ref,
            well_level_ref,
            well_pull_ref,
        ),
        (source_spot, first_amount, second_amount, well_spot, well_level, well_pull),
        done,
    )
    size, rows, depth = survey_ref.shape
    wide = (root_ref.shape[1], depth)
    place_x, even_x = place_in(GX)
    place_y, _ = place_in(GY)
    anchor_x = place_x * size
    anchor_y = place_y * rows

    spread(
        state_ref,
        RIM,
        Own((size, rows), lambda k: start_ref[k]),
        lambda k: x_one_ref[0, k],
        lambda k: x_two_ref[0, k],
        lambda k: y_one_ref[0, k],
        lambda k: y_two_ref[0, k],
    )
    spread(
        root_ref,
        RIM,
        Own((size, rows), lambda k: own_root_ref[k]),
        lambda k: jnp.exp(0.5 * x_one_ref[1, k]),
        lambda k: jnp.exp(0.5 * x_two_ref[1, k]),
        lambda k: jnp.exp(0.5 * y_one_ref[1, k]),
        lambda k: jnp.exp(0.5 * y_two_ref[1, k]),
    )
    row_ref[...] = row_mask(wide, anchor_y, grid_y)
    open_z = lane_mask(wide)

    def along_x(ref, plane):
        here = ref[plane]
        ahead = ref[plane + 1]
        cond = root_ref[plane] * root_ref[plane + 1]
        flux = head_slope * cond * here - (molecular + dispersivity * cond) * (ahead - here)
        return flux * plane_mask(plane, anchor_x, grid_x)

    def advanced(ref, plane):
        here = ref[plane]
        root = root_ref[plane]
        flux_x = along_x(ref, plane)
        cond_y = root * up(root, 0)
        flux_y = (row_ref[...] * (molecular + dispersivity * cond_y)) * (here - up(here, 0))
        cond_z = root * up(root, 1)
        flux_z = (open_z * (molecular + dispersivity * cond_z)) * (here - up(here, 1))
        change = (flux_x - flux_ref[...]) + (flux_y - down(flux_y, 0)) + (flux_z - down(flux_z, 1))
        flux_ref[...] = flux_x
        return here - change

    lane = lax.broadcasted_iota(jnp.int32, (1, depth), 1)

    flux_ref[...] = along_x(state_ref, 0)

    def first_step(plane, carry):
        next_ref[plane] = advanced(state_ref, plane)
        return carry

    lax.fori_loop(1, size + 2 * RIM - 1, first_step, 0)

    for copy in copies:
        copy.wait()

    sources = source_spot[source_spot.shape[0] - PAD]

    def add_first(index, carry):
        plane, row, at_z = unpack_spot(source_spot[index], depth)
        where = (plane, pl.ds(row, 1), slice(None))
        next_ref[where] = next_ref[where] + jnp.where(lane == at_z, first_amount[index], 0.0)
        return carry

    lax.fori_loop(0, sources, add_first, 0)

    flux_ref[...] = along_x(next_ref, RIM - 1)

    def second_step(k, carry):
        final_ref[k] = advanced(next_ref, k + RIM)[ROW : ROW + rows]
        return carry

    lax.fori_loop(0, size, second_step, 0)

    def add_second(index, carry):
        plane, row, at_z = unpack_spot(source_spot[index], depth)
        plane = plane - RIM
        row = row - ROW

        @pl.when((plane >= 0) & (plane < size) & (row >= 0) & (row < rows))
        def _():
            where = (plane, pl.ds(row, 1), slice(None))
            amount = second_amount[index]
            final_ref[where] = final_ref[where] + jnp.where(lane == at_z, amount, 0.0)

        return carry

    lax.fori_loop(0, sources, add_second, 0)

    def compare(k, total):
        missed = final_ref[k] - survey_ref[k]
        seed = weight_ref[k] * missed
        seed_ref[k] = seed
        return total + jnp.sum((seed * missed).reshape(rows // 8, 8, depth), axis=0)

    total = lax.fori_loop(0, size, compare, jnp.zeros((8, depth), jnp.float32))

    def observe(index, total):
        plane, row, at_z = unpack_spot(well_spot[index], depth)
        where = (plane - RIM, pl.ds(row - ROW, 1), slice(None))
        nearby = final_ref[where] - well_level[index]
        pull = jnp.where(lane == at_z, well_pull[index] * nearby, 0.0)
        seed_ref[where] = seed_ref[where] + pull
        return total + pull * nearby

    wells = well_spot[well_spot.shape[0] - PAD]
    total = lax.fori_loop(0, wells, observe, jnp.sum(total, axis=0, keepdims=True))
    total = total * (0.5 / (grid_x * grid_y * depth))
    for k in range(partial_ref.shape[0]):
        partial_ref[k] = total

    first = jnp.where(even_x, 0, size - RIM)
    second = size - RIM - first
    for k in range(RIM):
        edge_one_ref[k] = seed_ref[first + k]
        edge_two_ref[k] = seed_ref[second + k]


def adjoint_kernel(
    grid_x,
    grid_y,
    root_ref,
    state_ref,
    next_ref,
    seed_ref,
    x_one_ref,
    x_two_ref,
    y_one_ref,
    y_two_ref,
    grad_ref,
    back_ref,
    last_ref,
    middle_ref,
    partial_ref,
    row_ref,
    pull_ref,
    sens_ref,
):
    size, rows, depth = seed_ref.shape
    wide = (root_ref.shape[1], depth)
    place_x, _ = place_in(GX)
    place_y, _ = place_in(GY)
    anchor_x = place_x * size
    anchor_y = place_y * rows
    spread(
        last_ref,
        RIM,
        Own((size, rows), lambda k: seed_ref[k]),
        lambda k: x_one_ref[k],
        lambda k: x_two_ref[k],
        lambda k: y_one_ref[k],
        lambda k: y_two_ref[k],
    )
    row_ref[...] = row_mask(wide, anchor_y, grid_y)
    open_z = lane_mask(wide)

    def along_x(adjoint_ref, tracer_ref, plane):
        jump = plane_mask(plane, anchor_x, grid_x) * (adjoint_ref[plane + 1] - adjoint_ref[plane])
        cond = root_ref[plane] * root_ref[plane + 1]
        pull = jump * (molecular + dispersivity * cond)
        push = jump * (head_slope * cond) + pull
        here = tracer_ref[plane]
        rise = head_slope * here - dispersivity * (tracer_ref[plane + 1] - here)
        return push, pull, jump * rise * (0.5 * cond)

    def along(adjoint, tracer, root, is_open, axis):
        jump = is_open * (up(adjoint, axis) - adjoint)
        cond = root * up(root, axis)
        pull = jump * (molecular + dispersivity * cond)
        sens = (jump * (tracer - up(tracer, axis))) * ((0.5 * dispersivity) * cond)
        return pull - down(pull, axis), sens + down(sens, axis)

    def reversed_step(adjoint_ref, tracer_ref, plane):
        push, pull, sens = along_x(adjoint_ref, tracer_ref, plane)
        adjoint = adjoint_ref[plane]
        tracer = tracer_ref[plane]
        root = root_ref[plane]
        change_y, sens_y = along(adjoint, tracer, root, row_ref[...], 0)
        change_z, sens_z = along(adjoint, tracer, root, open_z, 1)
        updated = adjoint + (push - pull_ref[...]) + change_y + change_z
        gradient = (sens + sens_ref[...]) + sens_y + sens_z
        pull_ref[...] = pull
        sens_ref[...] = sens
        return updated, gradient

    def begin(adjoint_ref, tracer_ref, plane):
        _, pull, sens = along_x(adjoint_ref, tracer_ref, plane)
        pull_ref[...] = pull
        sens_ref[...] = sens

    begin(last_ref, next_ref, RIM - 2)

    def later(plane, carry):
        updated, gradient = reversed_step(last_ref, next_ref, plane)
        middle_ref[plane] = updated
        partial_ref[plane] = gradient
        return carry

    lax.fori_loop(RIM - 1, size + RIM + 1, later, 0)

    begin(middle_ref, state_ref, RIM - 1)

    def earlier(k, carry):
        updated, gradient = reversed_step(middle_ref, state_ref, k + RIM)
        back_ref[k] = updated[ROW : ROW + rows]
        grad_ref[k] = (gradient + partial_ref[k + RIM])[ROW : ROW + rows]
        return carry

    lax.fori_loop(0, size, earlier, 0)


def call(kernel, outs, operands, *, scratch=(), flops=1_000_000, limit=2):
    shapes = tuple(
        space(shape, jnp.float32)
        if space == pltpu.VMEM
        else jax.ShapeDtypeStruct(*shape)
        if space == pltpu.SMEM
        else jax.ShapeDtypeStruct(shape, jnp.float32)
        for shape, space in outs
    )
    arrays = [
        array if space == pltpu.SMEM else pltpu.with_memory_space_constraint(array, space)
        for array, space in operands
    ]
    out_spaces = [pltpu.VMEM if space is None else space for _, space in outs]
    return pl.pallas_call(
        kernel,
        out_shape=shapes,
        in_specs=[pl.BlockSpec(memory_space=space) for _, space in operands],
        out_specs=tuple(pl.BlockSpec(memory_space=space) for space in out_spaces),
        scratch_shapes=scratch,
        cost_estimate=pl.CostEstimate(flops=flops, transcendentals=0, bytes_accessed=1_000_000),
        compiler_params=pltpu.CompilerParams(vmem_limit_bytes=limit << 20),
    )(*arrays)


def kept(*arrays, space=pltpu.VMEM):
    return tuple((array, space) for array in arrays)


def swapped(one, two, axes):
    count = lax.axis_size(axes)
    outer = [(i, i + 1) for i in range(1, count - 1, 2)]
    inner = [(i, i + 1) for i in range(0, count - 1, 2)]
    back = lambda pairs: pairs + [(b, a) for a, b in pairs]
    one = lax.ppermute(one, axes, back(outer))
    two = lax.ppermute(two, axes, back(inner))
    return one, two


def on_device(
    log_cond,
    checkpoint,
    survey,
    survey_weight,
    well_cells,
    well_data,
    well_weight,
    source_cells,
    source_rate,
    step_number,
):
    size, rows, depth = checkpoint.shape
    grid_x = size * lax.axis_size(GX)
    grid_y = rows * lax.axis_size(GY)
    clock = step_number.astype(jnp.float32)
    first_factor = 1.0 + 0.5 * jnp.sin(0.05 * clock)
    second_factor = 1.0 + 0.5 * jnp.sin(0.05 * (clock + 1.0))

    planes = size + 2 * RIM
    wide = (planes, rows + 2 * ROW, depth)
    flat = wide[1:]
    block = (size, rows, depth)
    f32 = functools.partial(pltpu.VMEM, dtype=jnp.float32)
    dma = pltpu.SemaphoreType.DMA

    x_edge = (2, RIM, rows, depth)
    x_one, x_two = call(
        pack_x_kernel,
        kept(x_edge, x_edge),
        kept(checkpoint, log_cond, space=pltpu.HBM),
        scratch=[dma((4,))],
    )
    x_one, x_two = swapped(x_one, x_two, GX)

    sources = source_cells.shape[0] + PAD
    wells = well_cells.shape[0] + PAD

    def found(count):
        spaces = (((count,), jnp.int32), ((count,), jnp.float32), ((count,), jnp.float32))
        return kept(*spaces, space=pltpu.SMEM)

    def held(arrays):
        return [pltpu.SMEM(array.shape, array.dtype) for array in arrays] + [dma((len(arrays),))]

    source_lists = (source_cells, source_rate)
    well_lists = (well_cells, well_data, well_weight)
    root, *source_hits = call(
        functools.partial(lay_kernel, grid_y),
        kept(block) + found(sources),
        kept(first_factor, second_factor, space=pltpu.SMEM)
        + kept(*source_lists)
        + kept(log_cond),
        scratch=held(source_lists),
        flops=4_000_000,
    )
    well_hits = call(
        functools.partial(find_kernel, block, grid_y),
        found(wells),
        kept(*well_lists),
        scratch=held(well_lists),
        flops=4_000_000,
    )
    hits = (*source_hits, *well_hits)

    y_edge = (2, planes, RIM, depth)
    y_one, y_two = call(
        pack_y_kernel, kept(y_edge, y_edge), kept(checkpoint, log_cond, x_one, x_two)
    )
    y_one, y_two = swapped(y_one, y_two, GY)

    s_edge = (RIM, rows, depth)
    near_axes = ("gx_1", GY)
    near_count = lax.axis_size(near_axes)
    fields = (root, checkpoint, x_one, x_two, y_one, y_two, survey, survey_weight)
    root, state, later, final, seed, s_one, s_two, partial = call(
        functools.partial(forward_kernel, grid_x, grid_y),
        kept(wide, wide, wide)
        + kept(block, space=None)
        + kept(block, s_edge, s_edge, (near_count, 1, depth)),
        kept(*hits) + kept(*fields),
        scratch=[f32(flat), f32(flat)] + held(hits),
        flops=20_000_000,
        limit=4,
    )

    near = lax.all_to_all(partial, near_axes, 0, 0, tiled=True)
    (near,) = call(sum_kernel, kept((lax.axis_size(FAR), 1, depth)), kept(near))
    everyone = lax.all_to_all(near, FAR, 0, 0, tiled=True)
    misfit = jnp.sum(everyone).reshape(1)

    s_one, s_two = swapped(s_one, s_two, GX)
    t_edge = (planes, RIM, depth)
    t_one, t_two = call(pack_seed_kernel, kept(t_edge, t_edge), kept(seed, s_one, s_two))
    t_one, t_two = swapped(t_one, t_two, GY)
    grad, back = call(
        functools.partial(adjoint_kernel, grid_x, grid_y),
        kept(block, block, space=None),
        kept(root, state, later, seed, s_one, s_two, t_one, t_two),
        scratch=[f32(wide)] * 3 + [f32(flat)] * 3,
        flops=20_000_000,
        limit=6,
    )
    return (grad, back, final, misfit)


def solution(mesh):
    ens, along_x, along_y = (mesh.shape[name] for name in ("ens", "gx", "gy"))
    finer = Mesh(
        mesh.devices.reshape(ens, along_x // 2, 2, along_y), ("ens", "gx_0", "gx_1", "gy")
    )
    field = P(ENS_GX, "gy", None)

    return jax.shard_map(
        on_device,
        mesh=finer,
        in_specs=(field,) * 4 + (P("ens"),) * 6,
        out_specs=(field, field, field, P("ens")),
        check_vma=False,
    )
```
